512 devices in a mesh: grp: 64 (over x, z_hi, y), seg: 8 (over z_lo, core).
Axes of the slice: x: 4, y: 4, z: 16 (z_hi: 4, z_lo: 4; z = z_hi * 4 + z_lo), core: 2. Of those that a mesh axis runs over, the one named last changes fastest.
Arguments:
- queries: bfloat16 [524288, 384], P(('grp', 'seg')), may hold values from -16 to 16
- keys: bfloat16 [524288, 384], P(('grp', 'seg')), may hold values from -16 to 16
- values: bfloat16 [524288, 384], P(('grp', 'seg')), may hold values from -6 to 6
Outputs:
- attended: bfloat16 [524288, 384], P(('grp', 'seg'))
The draws below stay inside these ranges and needn't reach their ends.
All inputs are finite; a program needn't handle non-finite values.
Results may differ from the reference program's by a relative error of at most 0.0041.
Values may be sent and summed in bfloat16 or wider, within the bound.
No kernel may reach another device: no remote copies, remote signals or barrier semaphores. Data moves between devices by JAX's collectives and lax.ppermute only.
A program may use at most 64 MiB of HBM per device.

```python
import jax
import jax.numpy as jnp
from jax import lax

TOK_DEV = 1024
HEADS = 6
HEAD_WIDTH = 64
SLIDE_LENGTH = 131072
SLIDE_COUNT = 4
TOKEN_TOTAL = 524288
CENTER_DILATION = 8
SEGMENT_TOKENS = 8192
WIDE_DILATION = 128


def draw_queries(key, part):
    field = 1.5 * jax.random.normal(jax.random.fold_in(key, 11), (TOKEN_TOTAL, HEADS * HEAD_WIDTH), jnp.float32)
    return jnp.clip(field, -16.0, 16.0).astype(jnp.bfloat16)


def draw_keys(key, part):
    field = jax.random.normal(jax.random.fold_in(key, 13), (TOKEN_TOTAL, HEADS * HEAD_WIDTH), jnp.float32)
    return jnp.clip(field, -16.0, 16.0).astype(jnp.bfloat16)


def levels(rng, dims, shards, low, top_value):
    gain = 1.0
    for dim, parts in shards:
        draws = jax.random.uniform(jax.random.fold_in(jax.random.fold_in(rng, 6), dim), (parts,), jnp.float32, low / len(shards), top_value / len(shards))
        gain = gain * jnp.repeat(jnp.exp(draws), dims[dim] // parts).reshape((-1,) + (1,) * (len(dims) - 1 - dim))
    return gain


def gaussian(own_key, dims, scale, limit, cuts=(), held_as=jnp.bfloat16):
    factor_of = levels(own_key, dims, cuts, -0.22, 0.18) if cuts else 1.0
    result = jax.random.normal(own_key, dims, jnp.float32) * scale * factor_of
    return jnp.minimum(jnp.maximum(result, -limit), limit).astype(held_as)


def setup_inputs(seed: int = 0) -> dict:
    seeds = jax.random.split(jax.random.key(seed), 4)
    return {
        "queries": draw_queries(jax.random.fold_in(seeds[3], 71), 0),
        "keys": draw_keys(jax.random.fold_in(seeds[3], 71), 0),
        "values": gaussian(seeds[2], (TOKEN_TOTAL, HEADS * HEAD_WIDTH), 1.0, 6.0, ((0, 512),)),
    }


def attend(query_matrix, key_matrix, value_matrix):
    scores = jnp.einsum("...nd,...md->...nm", query_matrix.astype(jnp.float32), key_matrix.astype(jnp.float32)) * (HEAD_WIDTH ** -0.5)
    highest = jnp.max(scores, axis=-1, keepdims=True)
    raised = jnp.exp(scores - highest)
    totals = jnp.sum(raised, axis=-1)
    rounded_length = lax.optimization_barrier(raised.astype(jnp.bfloat16))
    mixed = jnp.einsum("...nm,...md->...nd", rounded_length.astype(jnp.float32), value_matrix.astype(jnp.float32)) / totals[..., None]
    return mixed, highest[..., 0] + jnp.log(totals)


def blend(near_out, near_lse, center_output, center_logsumexp, center_coverage, wide_output, wide_logsumexp, wide_coverage):
    mid_level = jnp.where(center_coverage, center_logsumexp, near_lse)
    far_level = jnp.where(wide_coverage, wide_logsumexp, near_lse)
    ceiling = jnp.maximum(jnp.maximum(near_lse, mid_level), far_level)
    near_weight = jnp.exp(near_lse - ceiling)
    mid_weight = jnp.where(center_coverage, jnp.exp(mid_level - ceiling), 0.0)
    far_weight = jnp.where(wide_coverage, jnp.exp(far_level - ceiling), 0.0)
    weighted = near_weight[..., None] * near_out + mid_weight[..., None] * center_output + far_weight[..., None] * wide_output
    return weighted / (near_weight + mid_weight + far_weight)[..., None]


def run_triple(triple):
    return attend(triple[0], triple[1], triple[2])


def reference(queries, keys, values):
    results = []
    center_segments = TOKEN_TOTAL // SEGMENT_TOKENS
    center_rows = SEGMENT_TOKENS // CENTER_DILATION
    wide_rows = TOKEN_TOTAL // WIDE_DILATION
    slide_wide_rows = SLIDE_LENGTH // WIDE_DILATION
    for index_of_head in range(HEADS):
        lower = index_of_head * HEAD_WIDTH
        upper = lower + HEAD_WIDTH
        query_head = queries[:, lower:upper]
        key_head = keys[:, lower:upper]
        value_head = values[:, lower:upper]

        def blocked(source_tensor):
            return source_tensor.reshape(TOKEN_TOTAL // TOK_DEV, TOK_DEV, HEAD_WIDTH)

        near_out, near_lse = lax.map(run_triple, (blocked(query_head), blocked(key_head), blocked(value_head)))
        near_out = near_out.reshape(TOKEN_TOTAL, HEAD_WIDTH)
        near_lse = near_lse.reshape(TOKEN_TOTAL)

        center_shift = index_of_head % CENTER_DILATION

        def middle(source_tensor):
            return source_tensor.reshape(center_segments, center_rows, CENTER_DILATION, HEAD_WIDTH)[:, :, center_shift]

        center_output, center_logsumexp = lax.map(run_triple, (middle(query_head), middle(key_head), middle(value_head)))
        center_flags = jnp.arange(CENTER_DILATION) == center_shift
        center_coverage = jnp.broadcast_to(center_flags, (center_segments, center_rows, CENTER_DILATION)).reshape(TOKEN_TOTAL)
        center_output_full = jnp.broadcast_to(center_output[:, :, None, :], (center_segments, center_rows, CENTER_DILATION, HEAD_WIDTH)).reshape(TOKEN_TOTAL, HEAD_WIDTH)
        center_logsumexp_full = jnp.broadcast_to(center_logsumexp[:, :, None], (center_segments, center_rows, CENTER_DILATION)).reshape(TOKEN_TOTAL)

        wide_shift = index_of_head % WIDE_DILATION

        def distant(source_tensor):
            return source_tensor.reshape(SLIDE_COUNT, slide_wide_rows, WIDE_DILATION, HEAD_WIDTH)[:, :, wide_shift]

        wide_output, wide_logsumexp = lax.map(run_triple, (distant(query_head), distant(key_head), distant(value_head)))
        wide_output = wide_output.reshape(wide_rows, HEAD_WIDTH)
        wide_logsumexp = wide_logsumexp.reshape(wide_rows)
        wide_flags = jnp.arange(WIDE_DILATION) == wide_shift
        wide_coverage = jnp.broadcast_to(wide_flags, (wide_rows, WIDE_DILATION)).reshape(TOKEN_TOTAL)
        wide_output_full = jnp.broadcast_to(wide_output[:, None, :], (wide_rows, WIDE_DILATION, HEAD_WIDTH)).reshape(TOKEN_TOTAL, HEAD_WIDTH)
        wide_logsumexp_full = jnp.broadcast_to(wide_logsumexp[:, None], (wide_rows, WIDE_DILATION)).reshape(TOKEN_TOTAL)

        results.append(blend(near_out, near_lse, center_output_full, center_logsumexp_full, center_coverage, wide_output_full, wide_logsumexp_full, wide_coverage))
    stacked = jnp.stack(results, axis=1)
    return stacked.reshape(TOKEN_TOTAL, HEADS * HEAD_WIDTH).astype(jnp.bfloat16)
```

```python
import jax
import jax.numpy as jnp
from jax import lax
from jax.experimental import pallas as pl
from jax.experimental.pallas import tpu as pltpu
from jax.sharding import PartitionSpec as P

HEADS = 6
HEAD_WIDTH = 64
PAIRS = HEADS // 2
LANES = 2 * HEAD_WIDTH
SLIDE_GRP = 16
SEG = 8
ROWS = 1024
MID = ROWS // SEG
FAR_PERIOD = SLIDE_GRP * SEG
FAR = ROWS // FAR_PERIOD
CHUNK = 256
SCALE = HEAD_WIDTH ** (-0.5)


NT = (((1,), (1,)), ((), ()))
NN = (((1,), (0,)), ((), ()))
TN = (((0,), (0,)), ((), ()))
F32 = jnp.float32
BF16 = jnp.bfloat16

SEND_MID = 224
BACK_MID = 80
BACK = BACK_MID + (PAIRS + 1) * FAR


def dot(a, b, dims):
    return lax.dot_general(a, b, dims, preferred_element_type=F32)


def lane_low(shape):
    return lax.broadcasted_iota(jnp.int32, shape, len(shape) - 1) < HEAD_WIDTH


def split3(x):
    high = x.astype(BF16)
    rest = x - high.astype(F32)
    middle = rest.astype(BF16)
    low = (rest - middle.astype(F32)).astype(BF16)
    return high, middle, low


def pack_kernel(q_ref, k_ref, v_ref, mid_ref, far_ref, q_wide, k_wide, v_wide):
    far_q, far_k, far_v = [], [], []
    low_mid = lane_low((MID, LANES))
    low_half = lane_low((MID // 2, LANES))
    low_far = lane_low((FAR, LANES))
    for pair in range(PAIRS):
        cols = slice(pair * LANES, (pair + 1) * LANES)
        q_wide[...] = q_ref[:, cols].astype(F32)
        k_wide[...] = k_ref[:, cols].astype(F32)
        v_wide[...] = v_ref[:, cols].astype(F32)
        for side in range(2):
            head = 2 * pair + side
            q_rows = q_wide[pl.ds(head, MID, stride=SEG), :]
            k_rows = k_wide[pl.ds(head, MID, stride=SEG), :]
            v_rows = v_wide[pl.ds(head, MID, stride=SEG), :]
            if side == 0:
                key_value = jnp.where(low_mid, k_rows, pltpu.roll(v_rows, HEAD_WIDTH, 1))
                query = jnp.where(
                    low_half, q_rows[: MID // 2], pltpu.roll(q_rows[MID // 2 :], HEAD_WIDTH, 1)
                )
            else:
                key_value = jnp.where(low_mid, pltpu.roll(k_rows, HEAD_WIDTH, 1), v_rows)
                query = jnp.where(
                    low_half, pltpu.roll(q_rows[: MID // 2], HEAD_WIDTH, 1), q_rows[MID // 2 :]
                )
            mid_ref[head, 0:MID, :] = key_value.astype(BF16)
            mid_ref[head, MID : MID + MID // 2, :] = query.astype(BF16)
        for wide, out in ((q_wide, far_q), (k_wide, far_k), (v_wide, far_v)):
            first = wide[pl.ds(2 * pair, FAR, stride=FAR_PERIOD), :]
            second = wide[pl.ds(2 * pair + 1, FAR, stride=FAR_PERIOD), :]
            out.append(jnp.where(low_far, first, second))
    for spare in range(HEADS, SEG):
        mid_ref[spare, 0 : MID + MID // 2, :] = jnp.zeros((MID + MID // 2, LANES), BF16)
    tail = jnp.concatenate(far_q + [jnp.zeros((FAR, LANES), F32)], axis=0).astype(BF16)
    for target in range(SEG):
        mid_ref[target, MID + MID // 2 : SEND_MID, :] = tail
    both = jnp.concatenate(far_k + far_v, axis=0).astype(BF16)
    for target in range(SLIDE_GRP):
        far_ref[target] = both


def pack(queries, keys, values):
    return pl.pallas_call(
        pack_kernel,
        out_shape=(
            jax.ShapeDtypeStruct((SEG, SEND_MID, LANES), BF16),
            jax.ShapeDtypeStruct((SLIDE_GRP, 2 * PAIRS * FAR, LANES), BF16),
        ),
        scratch_shapes=[pltpu.VMEM((ROWS, LANES), F32)] * 3,
        name="pack",
    )(queries, keys, values)


def scores_of(key_rows, query_rows):
    return dot(key_rows, query_rows, NT)


def finish(scores, value_columns):
    highest = jnp.max(scores, axis=0, keepdims=True)
    raised = jnp.exp(scores - highest).astype(BF16)
    mixed = dot(value_columns, raised, NN)
    totals = mixed[HEAD_WIDTH : HEAD_WIDTH + 1]
    return mixed[:HEAD_WIDTH] / totals, highest + jnp.log(totals)


def chunks_of(key_rows, query_parts, value_parts, put):
    count = len(query_parts)
    pending = scores_of(key_rows, query_parts[0]())
    for step in range(count):
        following = scores_of(key_rows, query_parts[step + 1]()) if step + 1 < count else None
        mixed, lse = finish(pending, value_parts[step])
        put(step, mixed, lse)
        pending = following


def near_kernel(q_ref, k_ref, v_ref, o_ref, l_ref):
    key_rows = k_ref[...]
    columns = v_ref[...].T
    ones = jnp.ones((16, ROWS), BF16)
    sides = [
        jnp.concatenate([columns[i * HEAD_WIDTH : (i + 1) * HEAD_WIDTH], ones], axis=0)
        for i in range(2)
    ]
    low = lane_low((CHUNK, LANES))
    per_side = ROWS // CHUNK

    def query_part(side, part):
        def get():
            rows = q_ref[part * CHUNK : (part + 1) * CHUNK, :] * BF16(SCALE)
            keep = low if side == 0 else jnp.logical_not(low)
            return jnp.where(keep, rows, BF16(0))

        return get

    def put(step, mixed, lse):
        side, part = step // per_side, step % per_side
        span = slice(part * CHUNK, (part + 1) * CHUNK)
        o_ref[side * HEAD_WIDTH : (side + 1) * HEAD_WIDTH, span] = mixed.astype(BF16)
        l_ref[0, side : side + 1, span] = lse

    chunks_of(
        key_rows,
        [query_part(s, p) for s in range(2) for p in range(per_side)],
        [sides[s] for s in range(2) for _ in range(per_side)],
        put,
    )


def near(queries, keys, values, first, count):
    spec = pl.BlockSpec((ROWS, LANES), lambda i: (0, i + first))
    return pl.pallas_call(
        near_kernel,
        grid=(count,),
        in_specs=[spec] * 3,
        out_specs=(
            pl.BlockSpec((LANES, ROWS), lambda i: (i, 0)),
            pl.BlockSpec((1, 8, ROWS), lambda i: (i, 0, 0)),
        ),
        out_shape=(
            jax.ShapeDtypeStruct((count * LANES, ROWS), BF16),
            jax.ShapeDtypeStruct((count, 8, ROWS), F32),
        ),
        cost_estimate=pl.CostEstimate(
            flops=count * 2 * 4 * ROWS * ROWS * HEAD_WIDTH,
            bytes_accessed=count * 4 * ROWS * LANES * 2,
            transcendentals=count * 2 * ROWS * ROWS,
        ),
        name="near",
    )(queries, keys, values)


def mid_kernel(r_ref, s_ref):
    key_value = r_ref[:, 0:MID, :].reshape(ROWS, LANES)
    columns = jnp.concatenate(
        [key_value.T[HEAD_WIDTH:], jnp.ones((16, ROWS), BF16)], axis=0
    )
    low = lane_low((MID // 2, LANES))

    def query_block(source):
        packed = r_ref[source, MID : MID + MID // 2, :].astype(F32) * SCALE
        first = jnp.where(low, packed, 0.0)
        second = jnp.where(low, pltpu.roll(packed, HEAD_WIDTH, 1), 0.0)
        return jnp.concatenate([first, second], axis=0).astype(BF16)

    def query_part(step):
        return lambda: jnp.concatenate([query_block(2 * step), query_block(2 * step + 1)], axis=0)

    def put(step, mixed, lse):
        parts = [part.astype(F32) for part in split3(lse)]
        block = jnp.concatenate(
            [mixed] + parts + [jnp.zeros((BACK_MID - HEAD_WIDTH - 3, CHUNK), F32)], axis=0
        ).astype(BF16)
        s_ref[2 * step] = block[:, :MID]
        s_ref[2 * step + 1] = block[:, MID:]

    steps = ROWS // CHUNK
    chunks_of(key_value, [query_part(s) for s in range(steps)], [columns] * steps, put)


def mid(received):
    return pl.pallas_call(
        mid_kernel,
        out_shape=jax.ShapeDtypeStruct((SEG, BACK_MID, MID), BF16),
        cost_estimate=pl.CostEstimate(
            flops=4 * ROWS * ROWS * HEAD_WIDTH,
            bytes_accessed=ROWS * LANES * 4,
            transcendentals=ROWS * ROWS,
        ),
        name="mid",
    )(received)


def far_kernel(r_ref, f_ref, m_ref, s_ref):
    queries = r_ref[:, MID + MID // 2 : SEND_MID, :].astype(F32) * SCALE
    others = f_ref[...].astype(F32)
    count = SEG * FAR
    low = lane_low((count, LANES))
    lane = lax.broadcasted_iota(jnp.int32, (count, LANES), 1)
    marks = jnp.zeros((count, LANES), F32)
    pieces = []
    for pair in range(PAIRS):
        rows = queries[:, pair * FAR : (pair + 1) * FAR, :].reshape(count, LANES)
        key_rows = (
            others[:, pair * FAR : (pair + 1) * FAR, :].reshape(SLIDE_GRP * FAR, LANES).astype(BF16)
        )
        value_rows = (
            others[:, (PAIRS + pair) * FAR : (PAIRS + pair + 1) * FAR, :]
            .reshape(SLIDE_GRP * FAR, LANES)
            .astype(BF16)
        )
        outs = []
        for side in range(2):
            keep = low if side == 0 else jnp.logical_not(low)
            scores = dot(jnp.where(keep, rows, 0.0).astype(BF16), key_rows, NT)
            highest = jnp.max(scores, axis=1, keepdims=True)
            raised = jnp.exp(scores - highest)
            totals = jnp.sum(raised, axis=1, keepdims=True)
            outs.append(dot(raised.astype(BF16), value_rows, NN) / totals)
            for place, part in enumerate(split3(highest + jnp.log(totals))):
                marks = jnp.where(
                    lane == 3 * (2 * pair + side) + place, part.astype(F32), marks
                )
        pieces.append(jnp.where(low, outs[0], outs[1]).reshape(SEG, FAR, LANES))
    pieces.append(marks.reshape(SEG, FAR, LANES))
    s_ref[:, BACK_MID:, :] = jnp.concatenate(pieces, axis=1).astype(BF16)
    s_ref[:, :BACK_MID, :] = m_ref[...]


def far(received, others, mid_part):
    return pl.pallas_call(
        far_kernel,
        out_shape=jax.ShapeDtypeStruct((SEG, BACK, LANES), BF16),
        name="far",
    )(received, others, mid_part)


def merge_kernel(*refs):
    n = (len(refs) - 2) // 2
    near_refs, lse_refs = refs[:n], refs[n : 2 * n]
    back_ref, out_ref = refs[2 * n :]
    width = HEADS * HEAD_WIDTH
    parts = back_ref[:, BACK_MID:, :].astype(F32)
    count = SEG * FAR
    marks = parts[:, PAIRS * FAR :, :].reshape(count, LANES).astype(BF16)
    source = lax.broadcasted_iota(jnp.int32, (LANES, width), 0)
    target = lax.broadcasted_iota(jnp.int32, (LANES, width), 1) // HEAD_WIDTH
    gather = jnp.logical_and(source >= 3 * target, source < 3 * target + 3).astype(BF16)
    lse_parts = dot(marks, gather, NN).reshape(SEG, FAR, width)
    far_parts = jnp.concatenate(
        [
            parts[:, pair * FAR : (pair + 1) * FAR, :].reshape(count, LANES)
            for pair in range(PAIRS)
        ],
        axis=1,
    ).reshape(SEG, FAR, width)
    top = jnp.max(lse_parts, axis=0)
    weights = jnp.exp(lse_parts - top[None])
    total = jnp.sum(weights, axis=0)
    far_out = jnp.sum(weights * far_parts, axis=0) / total
    far_lse = top + jnp.log(total)
    place = lax.broadcasted_iota(jnp.int32, (FAR, MID), 0) * (MID // FAR)
    lane = lax.broadcasted_iota(jnp.int32, (FAR, MID), 1)
    thin = (lane == place).astype(BF16)
    far_rows = jnp.concatenate([far_out] + [x.astype(F32) for x in split3(far_lse)], axis=1)
    far_wide = dot(far_rows.astype(BF16), thin, TN)
    has_far = lax.broadcasted_iota(jnp.int32, (1, MID), 1) % (MID // FAR) == 0
    slot = lax.broadcasted_iota(jnp.int32, (MID, ROWS), 0) * SEG
    token = lax.broadcasted_iota(jnp.int32, (MID, ROWS), 1)
    offset = token - slot
    phase = lax.broadcasted_iota(jnp.int32, (1, ROWS), 1) % SEG
    start = 0
    for ref, lse_ref in zip(near_refs, lse_refs):
        for pair in range(ref.shape[0] // LANES):
            sides = []
            for side in range(2):
                head = start + 2 * pair + side
                back = back_ref[head, :BACK_MID].astype(F32)
                mid_out = back[:HEAD_WIDTH]
                mid_lse = back[64:65] + back[65:66] + back[66:67]
                base = head * HEAD_WIDTH
                w_out = far_wide[base : base + HEAD_WIDTH]
                w_lse = (
                    far_wide[width + base : width + base + 1]
                    + far_wide[2 * width + base : 2 * width + base + 1]
                    + far_wide[3 * width + base : 3 * width + base + 1]
                )
                w_lse = jnp.where(has_far, w_lse, mid_lse)
                high = jnp.maximum(mid_lse, w_lse)
                w_mid = jnp.exp(mid_lse - high)
                w_far = jnp.where(has_far, jnp.exp(w_lse - high), 0.0)
                sums = w_mid + w_far
                joint = (w_mid * mid_out + w_far * w_out) / sums
                joint_lse = high + jnp.log(sums)
                block = jnp.concatenate(
                    [joint]
                    + [x.astype(F32) for x in split3(joint_lse)]
                    + [jnp.zeros((BACK_MID - HEAD_WIDTH - 3, MID), F32)],
                    axis=0,
                ).astype(BF16)
                spread = dot(block, (offset == head).astype(BF16), NN)
                near_lse = lse_ref[pair, side : side + 1, :]
                joint_wide = spread[64:65] + spread[65:66] + spread[66:67]
                covered = phase == head
                joint_wide = jnp.where(covered, joint_wide, near_lse)
                ceiling = jnp.maximum(near_lse, joint_wide)
                near_weight = jnp.exp(near_lse - ceiling)
                joint_weight = jnp.where(covered, jnp.exp(joint_wide - ceiling), 0.0)
                share = joint_weight / (near_weight + joint_weight)
                rest = near_weight / (near_weight + joint_weight)
                own = ref[
                    pair * LANES + side * HEAD_WIDTH : pair * LANES + (side + 1) * HEAD_WIDTH, :
                ].astype(F32)
                sides.append(rest * own + share * spread[:HEAD_WIDTH])
            whole = start // 2 + pair
            out_ref[:, whole * LANES : (whole + 1) * LANES] = (
                jnp.concatenate(sides, axis=0).astype(BF16).T
            )
        start += 2 * (ref.shape[0] // LANES)


def merge(near_outs, near_lses, back):
    return pl.pallas_call(
        merge_kernel,
        out_shape=jax.ShapeDtypeStruct((ROWS, HEADS * HEAD_WIDTH), BF16),
        name="merge",
    )(*near_outs, *near_lses, back)


def body(queries, keys, values):
    groups = lax.axis_size("grp") // SLIDE_GRP
    slides = [[s * SLIDE_GRP + i for i in range(SLIDE_GRP)] for s in range(groups)]
    mid_send, far_send = pack(queries, keys, values)
    mid_got = lax.all_to_all(mid_send, "seg", 0, 0, tiled=True)
    far_got = lax.all_to_all(
        far_send, "grp", 0, 0, tiled=True, axis_index_groups=slides
    )
    nears = []
    for pair in range(3):
        nears.append(near(queries, keys, values, pair, 1))
    mid_part = mid(mid_got)
    part = far(mid_got, far_got, mid_part)
    back = lax.all_to_all(part, "seg", 0, 0, tiled=True)
    return merge([n[0] for n in nears], [n[1] for n in nears], back)


def solution(mesh):
    return jax.shard_map(
        body,
        mesh=mesh,
        in_specs=(P(("grp", "seg"), None),) * 3,
        out_specs=P(("grp", "seg"), None),
        check_vma=False,
    )
```

```python
import jax
import jax.numpy as jnp
from jax import lax
from jax.experimental import pallas as pl
from jax.experimental.pallas import tpu as pltpu
from jax.sharding import PartitionSpec as P

HEADS = 6
HEAD_WIDTH = 64
PAIRS = HEADS // 2
LANES = 2 * HEAD_WIDTH
SLIDE_GRP = 16
SEG = 8
ROWS = 1024
MID = ROWS // SEG
FAR_PERIOD = SLIDE_GRP * SEG
FAR = ROWS // FAR_PERIOD
CHUNK = 256
SCALE = HEAD_WIDTH ** (-0.5)


NT = (((1,), (1,)), ((), ()))
NN = (((1,), (0,)), ((), ()))
TN = (((0,), (0,)), ((), ()))
F32 = jnp.float32
BF16 = jnp.bfloat16

SEND_MID = 224
BACK_MID = 80
BACK = BACK_MID + (PAIRS + 1) * FAR


def held_call(kernel, out_shapes, *operands, room=8, **options):
    outs = tuple(pltpu.VMEM(shape, dtype) for shape, dtype in out_shapes)
    space = pl.BlockSpec(memory_space=pltpu.VMEM)
    return pl.pallas_call(
        kernel,
        out_shape=outs,
        in_specs=[space] * len(operands),
        out_specs=(space,) * len(outs),
        compiler_params=pltpu.CompilerParams(vmem_limit_bytes=room * 2**20),
        **options,
    )(*[pltpu.with_memory_space_constraint(x, pltpu.VMEM) for x in operands])


def dot(a, b, dims):
    return lax.dot_general(a, b, dims, preferred_element_type=F32)


def lane_low(shape):
    return lax.broadcasted_iota(jnp.int32, shape, len(shape) - 1) < HEAD_WIDTH


def split3(x):
    high = x.astype(BF16)
    rest = x - high.astype(F32)
    middle = rest.astype(BF16)
    low = (rest - middle.astype(F32)).astype(BF16)
    return high, middle, low


def pack_kernel(*refs):
    sources, refs = refs[:3], refs[3:]
    mid_ref, far_ref = refs[:2]
    copies, (q_wide, k_wide, v_wide, sems) = refs[2:-4], refs[-4:]
    moves = []
    for pair in range(PAIRS):
        for place, source in enumerate(sources):
            slot = 3 * pair + place
            move = pltpu.make_async_copy(
                source.at[:, pair * LANES : (pair + 1) * LANES], copies[slot], sems.at[slot]
            )
            move.start()
            moves.append(move)
    far_q, far_k, far_v = [], [], []
    low_mid = lane_low((MID, LANES))
    low_half = lane_low((MID // 2, LANES))
    low_far = lane_low((FAR, LANES))
    for spare in range(HEADS, SEG):
        mid_ref[spare, 0 : MID + MID // 2, :] = jnp.zeros((MID + MID // 2, LANES), BF16)
    for pair in range(PAIRS):
        for place, wide in enumerate((q_wide, k_wide, v_wide)):
            moves[3 * pair + place].wait()
            wide[...] = copies[3 * pair + place][...].astype(F32)
        for side in range(2):
            head = 2 * pair + side
            q_rows = q_wide[pl.ds(head, MID, stride=SEG), :]
            k_rows = k_wide[pl.ds(head, MID, stride=SEG), :]
            v_rows = v_wide[pl.ds(head, MID, stride=SEG), :]
            if side == 0:
                key_value = jnp.where(low_mid, k_rows, pltpu.roll(v_rows, HEAD_WIDTH, 1))
                query = jnp.where(
                    low_half, q_rows[: MID // 2], pltpu.roll(q_rows[MID // 2 :], HEAD_WIDTH, 1)
                )
            else:
                key_value = jnp.where(low_mid, pltpu.roll(k_rows, HEAD_WIDTH, 1), v_rows)
                query = jnp.where(
                    low_half, pltpu.roll(q_rows[: MID // 2], HEAD_WIDTH, 1), q_rows[MID // 2 :]
                )
            mid_ref[head, 0:MID, :] = key_value.astype(BF16)
            mid_ref[head, MID : MID + MID // 2, :] = query.astype(BF16)
        for wide, out in ((q_wide, far_q), (k_wide, far_k), (v_wide, far_v)):
            first = wide[pl.ds(2 * pair, FAR, stride=FAR_PERIOD), :]
            second = wide[pl.ds(2 * pair + 1, FAR, stride=FAR_PERIOD), :]
            out.append(jnp.where(low_far, first, second))
    tail = jnp.concatenate(far_q + [jnp.zeros((FAR, LANES), F32)], axis=0).astype(BF16)
    for target in range(SEG):
        mid_ref[target, MID + MID // 2 : SEND_MID, :] = tail
    far_ref[0] = jnp.concatenate(far_k + far_v, axis=0).astype(BF16)


def pack(queries, keys, values):
    shapes = [((SEG, SEND_MID, LANES), BF16), ((1, 2 * PAIRS * FAR, LANES), BF16)]
    shapes += [((ROWS, LANES), BF16)] * (3 * PAIRS)
    space = pl.BlockSpec(memory_space=pltpu.VMEM)
    return pl.pallas_call(
        pack_kernel,
        out_shape=tuple(pltpu.VMEM(shape, dtype) for shape, dtype in shapes),
        in_specs=[pl.BlockSpec(memory_space=pl.ANY)] * 3,
        out_specs=(space,) * len(shapes),
        scratch_shapes=[pltpu.VMEM((ROWS, LANES), F32)] * 3
        + [pltpu.SemaphoreType.DMA((3 * PAIRS,))],
        compiler_params=pltpu.CompilerParams(vmem_limit_bytes=8 * 2**20),
        name="pack",
    )(*[pltpu.with_memory_space_constraint(x, pltpu.HBM) for x in (queries, keys, values)])


def scores_of(key_rows, query_rows):
    return dot(key_rows, query_rows, NT)


def finish(scores, value_columns):
    highest = jnp.max(scores, axis=0, keepdims=True)
    raised = jnp.exp(scores - highest).astype(BF16)
    mixed = dot(value_columns, raised, NN)
    totals = mixed[HEAD_WIDTH : HEAD_WIDTH + 1]
    return mixed[:HEAD_WIDTH] / totals, highest + jnp.log(totals)


def chunks_of(key_rows, query_parts, value_parts, put):
    count = len(query_parts)
    pending = scores_of(key_rows, query_parts[0]())
    for step in range(count):
        following = scores_of(key_rows, query_parts[step + 1]()) if step + 1 < count else None
        mixed, lse = finish(pending, value_parts[step])
        put(step, mixed, lse)
        pending = following


def near_kernel(q_ref, k_ref, v_ref, o_ref, l_ref):
    key_rows = k_ref[...]
    columns = v_ref[...].T
    ones = jnp.ones((16, ROWS), BF16)
    sides = [
        jnp.concatenate([columns[i * HEAD_WIDTH : (i + 1) * HEAD_WIDTH], ones], axis=0)
        for i in range(2)
    ]
    low = lane_low((CHUNK, LANES))
    per_side = ROWS // CHUNK

    def query_part(side, part):
        def get():
            rows = q_ref[part * CHUNK : (part + 1) * CHUNK, :] * BF16(SCALE)
            keep = low if side == 0 else jnp.logical_not(low)
            return jnp.where(keep, rows, BF16(0))

        return get

    def put(step, mixed, lse):
        side, part = step // per_side, step % per_side
        span = slice(part * CHUNK, (part + 1) * CHUNK)
        o_ref[side * HEAD_WIDTH : (side + 1) * HEAD_WIDTH, span] = mixed.astype(BF16)
        l_ref[0, side : side + 1, span] = lse

    chunks_of(
        key_rows,
        [query_part(s, p) for s in range(2) for p in range(per_side)],
        [sides[s] for s in range(2) for _ in range(per_side)],
        put,
    )


def near(queries, keys, values):
    return held_call(
        near_kernel,
        [((LANES, ROWS), BF16), ((1, 8, ROWS), F32)],
        queries,
        keys,
        values,
        cost_estimate=pl.CostEstimate(
            flops=2 * 4 * ROWS * ROWS * HEAD_WIDTH,
            bytes_accessed=4 * ROWS * LANES * 2,
            transcendentals=2 * ROWS * ROWS,
        ),
        room=16,
        name="near",
    )


def mid_kernel(r_ref, s_ref):
    key_value = r_ref[:, 0:MID, :].reshape(ROWS, LANES)
    columns = jnp.concatenate(
        [key_value.T[HEAD_WIDTH:], jnp.ones((16, ROWS), BF16)], axis=0
    )
    low = lane_low((MID // 2, LANES))

    def query_block(source):
        packed = r_ref[source, MID : MID + MID // 2, :].astype(F32) * SCALE
        first = jnp.where(low, packed, 0.0)
        second = jnp.where(low, pltpu.roll(packed, HEAD_WIDTH, 1), 0.0)
        return jnp.concatenate([first, second], axis=0).astype(BF16)

    def query_part(step):
        return lambda: jnp.concatenate([query_block(2 * step), query_block(2 * step + 1)], axis=0)

    def put(step, mixed, lse):
        parts = [part.astype(F32) for part in split3(lse)]
        block = jnp.concatenate(
            [mixed] + parts + [jnp.zeros((BACK_MID - HEAD_WIDTH - 3, CHUNK), F32)], axis=0
        ).astype(BF16)
        s_ref[2 * step] = block[:, :MID]
        s_ref[2 * step + 1] = block[:, MID:]

    steps = ROWS // CHUNK
    chunks_of(key_value, [query_part(s) for s in range(steps)], [columns] * steps, put)


def mid(received):
    return held_call(
        mid_kernel,
        [((SEG, BACK_MID, MID), BF16)],
        received,
        cost_estimate=pl.CostEstimate(
            flops=4 * ROWS * ROWS * HEAD_WIDTH,
            bytes_accessed=ROWS * LANES * 4,
            transcendentals=ROWS * ROWS,
        ),
        room=16,
        name="mid",
    )[0]


def far_kernel(r_ref, *refs):
    m_ref, s_ref = refs[-2:]
    queries = r_ref[:, MID + MID // 2 : SEND_MID, :].astype(F32) * SCALE
    others = jnp.concatenate([ref[...] for ref in refs[:-2]], axis=0).astype(F32)
    count = SEG * FAR
    low = lane_low((count, LANES))
    lane = lax.broadcasted_iota(jnp.int32, (count, LANES), 1)
    marks = jnp.zeros((count, LANES), F32)
    pieces = []
    for pair in range(PAIRS):
        rows = queries[:, pair * FAR : (pair + 1) * FAR, :].reshape(count, LANES)
        key_rows = (
            others[:, pair * FAR : (pair + 1) * FAR, :].reshape(SLIDE_GRP * FAR, LANES).astype(BF16)
        )
        value_rows = (
            others[:, (PAIRS + pair) * FAR : (PAIRS + pair + 1) * FAR, :]
            .reshape(SLIDE_GRP * FAR, LANES)
            .astype(BF16)
        )
        outs = []
        for side in range(2):
            keep = low if side == 0 else jnp.logical_not(low)
            scores = dot(jnp.where(keep, rows, 0.0).astype(BF16), key_rows, NT)
            highest = jnp.max(scores, axis=1, keepdims=True)
            raised = jnp.exp(scores - highest)
            totals = jnp.sum(raised, axis=1, keepdims=True)
            outs.append(dot(raised.astype(BF16), value_rows, NN) / totals)
            for place, part in enumerate(split3(highest + jnp.log(totals))):
                marks = jnp.where(
                    lane == 3 * (2 * pair + side) + place, part.astype(F32), marks
                )
        pieces.append(jnp.where(low, outs[0], outs[1]).reshape(SEG, FAR, LANES))
    pieces.append(marks.reshape(SEG, FAR, LANES))
    s_ref[:, BACK_MID:, :] = jnp.concatenate(pieces, axis=1).astype(BF16)
    s_ref[:, :BACK_MID, :] = m_ref[...]


def far(received, others, mid_part):
    return held_call(
        far_kernel, [((SEG, BACK, LANES), BF16)], received, *others, mid_part, name="far"
    )[0]


def merge_kernel(*refs):
    near_refs, lse_refs = refs[:PAIRS], refs[PAIRS : 2 * PAIRS]
    back_ref, out_ref, stage_ref, sems = refs[2 * PAIRS :]
    moves = []
    width = HEADS * HEAD_WIDTH
    parts = back_ref[:, BACK_MID:, :].astype(F32)
    count = SEG * FAR
    marks = parts[:, PAIRS * FAR :, :].reshape(count, LANES).astype(BF16)
    source = lax.broadcasted_iota(jnp.int32, (LANES, width), 0)
    target = lax.broadcasted_iota(jnp.int32, (LANES, width), 1) // HEAD_WIDTH
    gather = jnp.logical_and(source >= 3 * target, source < 3 * target + 3).astype(BF16)
    lse_parts = dot(marks, gather, NN).reshape(SEG, FAR, width)
    far_parts = jnp.concatenate(
        [
            parts[:, pair * FAR : (pair + 1) * FAR, :].reshape(count, LANES)
            for pair in range(PAIRS)
        ],
        axis=1,
    ).reshape(SEG, FAR, width)
    top = jnp.max(lse_parts, axis=0)
    weights = jnp.exp(lse_parts - top[None])
    total = jnp.sum(weights, axis=0)
    far_out = jnp.sum(weights * far_parts, axis=0) / total
    far_lse = top + jnp.log(total)
    place = lax.broadcasted_iota(jnp.int32, (FAR, MID), 0) * (MID // FAR)
    lane = lax.broadcasted_iota(jnp.int32, (FAR, MID), 1)
    thin = (lane == place).astype(BF16)
    far_rows = jnp.concatenate([far_out] + [x.astype(F32) for x in split3(far_lse)], axis=1)
    far_wide = dot(far_rows.astype(BF16), thin, TN)
    has_far = lax.broadcasted_iota(jnp.int32, (1, MID), 1) % (MID // FAR) == 0
    slot = lax.broadcasted_iota(jnp.int32, (MID, ROWS), 0) * SEG
    token = lax.broadcasted_iota(jnp.int32, (MID, ROWS), 1)
    offset = token - slot
    phase = lax.broadcasted_iota(jnp.int32, (1, ROWS), 1) % SEG
    start = 0
    for ref, lse_ref in zip(near_refs, lse_refs):
        for pair in range(ref.shape[0] // LANES):
            sides = []
            for side in range(2):
                head = start + 2 * pair + side
                back = back_ref[head, :BACK_MID].astype(F32)
                mid_out = back[:HEAD_WIDTH]
                mid_lse = back[64:65] + back[65:66] + back[66:67]
                base = head * HEAD_WIDTH
                w_out = far_wide[base : base + HEAD_WIDTH]
                w_lse = (
                    far_wide[width + base : width + base + 1]
                    + far_wide[2 * width + base : 2 * width + base + 1]
                    + far_wide[3 * width + base : 3 * width + base + 1]
                )
                w_lse = jnp.where(has_far, w_lse, mid_lse)
                high = jnp.maximum(mid_lse, w_lse)
                w_mid = jnp.exp(mid_lse - high)
                w_far = jnp.where(has_far, jnp.exp(w_lse - high), 0.0)
                sums = w_mid + w_far
                joint = (w_mid * mid_out + w_far * w_out) / sums
                joint_lse = high + jnp.log(sums)
                block = jnp.concatenate(
                    [joint]
                    + [x.astype(F32) for x in split3(joint_lse)]
                    + [jnp.zeros((BACK_MID - HEAD_WIDTH - 3, MID), F32)],
                    axis=0,
                ).astype(BF16)
                spread = dot(block, (offset == head).astype(BF16), NN)
                near_lse = lse_ref[pair, side : side + 1, :]
                joint_wide = spread[64:65] + spread[65:66] + spread[66:67]
                covered = phase == head
                joint_wide = jnp.where(covered, joint_wide, near_lse)
                ceiling = jnp.maximum(near_lse, joint_wide)
                near_weight = jnp.exp(near_lse - ceiling)
                joint_weight = jnp.where(covered, jnp.exp(joint_wide - ceiling), 0.0)
                share = joint_weight / (near_weight + joint_weight)
                rest = near_weight / (near_weight + joint_weight)
                own = ref[
                    pair * LANES + side * HEAD_WIDTH : pair * LANES + (side + 1) * HEAD_WIDTH, :
                ].astype(F32)
                sides.append(rest * own + share * spread[:HEAD_WIDTH])
            whole = start // 2 + pair
            stage_ref[whole] = jnp.concatenate(sides, axis=0).astype(BF16).T
            move = pltpu.make_async_copy(
                stage_ref.at[whole],
                out_ref.at[:, whole * LANES : (whole + 1) * LANES],
                sems.at[whole],
            )
            move.start()
            moves.append(move)
        start += 2 * (ref.shape[0] // LANES)
    for move in moves:
        move.wait()


def merge(near_outs, near_lses, back):
    operands = (*near_outs, *near_lses, back)
    return pl.pallas_call(
        merge_kernel,
        out_shape=jax.ShapeDtypeStruct((ROWS, HEADS * HEAD_WIDTH), BF16),
        in_specs=[pl.BlockSpec(memory_space=pltpu.VMEM)] * len(operands),
        out_specs=pl.BlockSpec(memory_space=pl.ANY),
        scratch_shapes=[
            pltpu.VMEM((PAIRS, ROWS, LANES), BF16),
            pltpu.SemaphoreType.DMA((PAIRS,)),
        ],
        compiler_params=pltpu.CompilerParams(vmem_limit_bytes=16 * 2**20),
        name="merge",
    )(*[pltpu.with_memory_space_constraint(x, pltpu.VMEM) for x in operands])


def fan_out(held, masks):
    size = lax.axis_size("grp")
    got = []
    for mask in masks:
        got.append(lax.ppermute(held, "grp", [(i, i ^ mask) for i in range(size)]))
    return got


def body(queries, keys, values):
    mid_send, held, *pieces = pack(queries, keys, values)
    mid_got = lax.all_to_all(mid_send, "seg", 0, 0, tiled=True)
    for mask in (8, 4):
        held = jnp.concatenate([held] + fan_out(held, (mask,)), axis=0)
    inner = fan_out(held, (1, 3, 2))
    nears = []
    for pair in range(3):
        nears.append(near(*pieces[3 * pair : 3 * pair + 3]))
    mid_part = mid(mid_got)
    part = far(mid_got, (held, *inner), mid_part)
    back = lax.all_to_all(part, "seg", 0, 0, tiled=True)
    return merge([n[0] for n in nears], [n[1] for n in nears], back)


def solution(mesh):
    return jax.shard_map(
        body,
        mesh=mesh,
        in_specs=(P(("grp", "seg"), None),) * 3,
        out_specs=P(("grp", "seg"), None),
        check_vma=False,
    )
```

```python
import jax
import jax.numpy as jnp
from jax import lax
from jax.experimental import pallas as pl
from jax.experimental.pallas import tpu as pltpu
from jax.sharding import PartitionSpec as P

HEADS = 6
HEAD_WIDTH = 64
PAIRS = HEADS // 2
LANES = 2 * HEAD_WIDTH
SLIDE_GRP = 16
SEG = 8
ROWS = 1024
MID = ROWS // SEG
FAR_PERIOD = SLIDE_GRP * SEG
FAR = ROWS // FAR_PERIOD
CHUNK = 256
BLOCK = 256
SCALE = HEAD_WIDTH ** (-0.5)


NT = (((1,), (1,)), ((), ()))
NN = (((1,), (0,)), ((), ()))
TN = (((0,), (0,)), ((), ()))
F32 = jnp.float32
BF16 = jnp.bfloat16

SEND_MID = 216
BACK_MID = 72
BACK = BACK_MID + (PAIRS + 1) * FAR


def held_call(kernel, out_shapes, *operands, room=8, **options):
    outs = tuple(pltpu.VMEM(shape, dtype) for shape, dtype in out_shapes)
    space = pl.BlockSpec(memory_space=pltpu.VMEM)
    return pl.pallas_call(
        kernel,
        out_shape=outs,
        in_specs=[space] * len(operands),
        out_specs=(space,) * len(outs),
        compiler_params=pltpu.CompilerParams(vmem_limit_bytes=room * 2**20),
        **options,
    )(*[pltpu.with_memory_space_constraint(x, pltpu.VMEM) for x in operands])


def dot(a, b, dims):
    return lax.dot_general(a, b, dims, preferred_element_type=F32)


def lane_low(shape):
    return lax.broadcasted_iota(jnp.int32, shape, len(shape) - 1) < HEAD_WIDTH


def split3(x):
    high = x.astype(BF16)
    rest = x - high.astype(F32)
    middle = rest.astype(BF16)
    low = (rest - middle.astype(F32)).astype(BF16)
    return high, middle, low


def pack_far_kernel(k_ref, v_ref, far_ref, taken, wide, sems):
    moves = []
    for place, source in enumerate((k_ref, v_ref)):
        move = pltpu.make_async_copy(source.at[:, 0:SEG, :], taken.at[place], sems.at[place])
        move.start()
        moves.append(move)
    low = lane_low((FAR, LANES))
    rows = []
    for place, move in enumerate(moves):
        move.wait()
        for pair in range(PAIRS):
            lanes = slice(pair * LANES, (pair + 1) * LANES)
            wide[...] = taken[place, :, :, lanes].astype(F32).reshape(FAR * SEG, LANES)
            first = wide[pl.ds(2 * pair, FAR, stride=SEG), :]
            second = wide[pl.ds(2 * pair + 1, FAR, stride=SEG), :]
            rows.append(jnp.where(low, first, second))
    far_ref[0] = jnp.concatenate(rows, axis=0).astype(BF16)


def pack_far(keys, values):
    width = HEADS * HEAD_WIDTH
    operands = [x.reshape(FAR, FAR_PERIOD, width) for x in (keys, values)]
    return pl.pallas_call(
        pack_far_kernel,
        out_shape=pltpu.VMEM((1, 2 * PAIRS * FAR, LANES), BF16),
        in_specs=[pl.BlockSpec(memory_space=pl.ANY)] * 2,
        out_specs=pl.BlockSpec(memory_space=pltpu.VMEM),
        scratch_shapes=[
            pltpu.VMEM((2, FAR, SEG, width), BF16),
            pltpu.VMEM((FAR * SEG, LANES), F32),
            pltpu.SemaphoreType.DMA((2,)),
        ],
        compiler_params=pltpu.CompilerParams(vmem_limit_bytes=4 * 2**20),
        name="pack_far",
    )(*[pltpu.with_memory_space_constraint(x, pltpu.HBM) for x in operands])


def pack_kernel(*refs):
    sources, refs = refs[:3], refs[3:]
    mid_ref, copies, (q_wide, k_wide, v_wide, sems) = refs[0], refs[1:-4], refs[-4:]
    moves = []
    for pair in range(PAIRS):
        for place, source in enumerate(sources):
            slot = 3 * pair + place
            move = pltpu.make_async_copy(
                source.at[:, pair * LANES : (pair + 1) * LANES], copies[slot], sems.at[slot]
            )
            move.start()
            moves.append(move)
    far_q = []
    low_mid = lane_low((MID, LANES))
    low_half = lane_low((MID // 2, LANES))
    low_far = lane_low((FAR, LANES))
    for spare in range(HEADS, SEG):
        mid_ref[spare, 0 : MID + MID // 2, :] = jnp.zeros((MID + MID // 2, LANES), BF16)
    for pair in range(PAIRS):
        for place, wide in enumerate((q_wide, k_wide, v_wide)):
            moves[3 * pair + place].wait()
            wide[...] = copies[3 * pair + place][...].astype(F32)
        for side in range(2):
            head = 2 * pair + side
            q_rows = q_wide[pl.ds(head, MID, stride=SEG), :]
            k_rows = k_wide[pl.ds(head, MID, stride=SEG), :]
            v_rows = v_wide[pl.ds(head, MID, stride=SEG), :]
            if side == 0:
                key_value = jnp.where(low_mid, k_rows, pltpu.roll(v_rows, HEAD_WIDTH, 1))
                query = jnp.where(
                    low_half, q_rows[: MID // 2], pltpu.roll(q_rows[MID // 2 :], HEAD_WIDTH, 1)
                )
            else:
                key_value = jnp.where(low_mid, pltpu.roll(k_rows, HEAD_WIDTH, 1), v_rows)
                query = jnp.where(
                    low_half, pltpu.roll(q_rows[: MID // 2], HEAD_WIDTH, 1), q_rows[MID // 2 :]
                )
            mid_ref[head, 0:MID, :] = key_value.astype(BF16)
            mid_ref[head, MID : MID + MID // 2, :] = query.astype(BF16)
        first = q_wide[pl.ds(2 * pair, FAR, stride=FAR_PERIOD), :]
        second = q_wide[pl.ds(2 * pair + 1, FAR, stride=FAR_PERIOD), :]
        far_q.append(jnp.where(low_far, first, second))
    tail = jnp.concatenate(far_q, axis=0).astype(BF16)
    for target in range(SEG):
        mid_ref[target, MID + MID // 2 : SEND_MID, :] = tail


def pack(queries, keys, values):
    shapes = [((SEG, SEND_MID, LANES), BF16)] + [((ROWS, LANES), BF16)] * (3 * PAIRS)
    space = pl.BlockSpec(memory_space=pltpu.VMEM)
    return pl.pallas_call(
        pack_kernel,
        out_shape=tuple(pltpu.VMEM(shape, dtype) for shape, dtype in shapes),
        in_specs=[pl.BlockSpec(memory_space=pl.ANY)] * 3,
        out_specs=(space,) * len(shapes),
        scratch_shapes=[pltpu.VMEM((ROWS, LANES), F32)] * 3
        + [pltpu.SemaphoreType.DMA((3 * PAIRS,))],
        compiler_params=pltpu.CompilerParams(vmem_limit_bytes=8 * 2**20),
        name="pack",
    )(*[pltpu.with_memory_space_constraint(x, pltpu.HBM) for x in (queries, keys, values)])


def chunks_of(key_rows, query_parts, value_parts, put):
    count = len(query_parts)
    blocks = [slice(at, at + BLOCK) for at in range(0, ROWS, BLOCK)]

    def top_of(tiles):
        best = tiles[0]
        for tile in tiles[1:]:
            best = jnp.maximum(best, tile)
        return jnp.max(best, axis=0, keepdims=True)

    query = query_parts[0]()
    pending = [dot(key_rows[block], query, NT) for block in blocks]
    for step in range(count):
        highest = top_of(pending)
        query = query_parts[step + 1]() if step + 1 < count else None
        following, mixed = [], None
        raised = []
        for block, tile in zip(blocks, pending):
            if query is not None:
                following.append(dot(key_rows[block], query, NT))
            raised.append(jnp.exp(tile - highest).astype(BF16))
        mixed = dot(value_parts[step], jnp.concatenate(raised, axis=0), NN)
        totals = mixed[HEAD_WIDTH : HEAD_WIDTH + 1]
        put(step, mixed[:HEAD_WIDTH] / totals, highest + jnp.log(totals))
        pending = following


def near_kernel(q_ref, k_ref, v_ref, o_ref, l_ref):
    key_rows = k_ref[...]
    columns = v_ref[...].T
    ones = jnp.ones((16, ROWS), BF16)
    sides = [
        jnp.concatenate([columns[i * HEAD_WIDTH : (i + 1) * HEAD_WIDTH], ones], axis=0)
        for i in range(2)
    ]
    low = lane_low((CHUNK, LANES))
    per_side = ROWS // CHUNK

    def query_part(side, part):
        def get():
            rows = q_ref[part * CHUNK : (part + 1) * CHUNK, :] * BF16(SCALE)
            keep = low if side == 0 else jnp.logical_not(low)
            return jnp.where(keep, rows, BF16(0))

        return get

    def put(step, mixed, lse):
        side, part = step // per_side, step % per_side
        span = slice(part * CHUNK, (part + 1) * CHUNK)
        o_ref[side * HEAD_WIDTH : (side + 1) * HEAD_WIDTH, span] = mixed.astype(BF16)
        l_ref[0, side : side + 1, span] = lse

    chunks_of(
        key_rows,
        [query_part(s, p) for s in range(2) for p in range(per_side)],
        [sides[s] for s in range(2) for _ in range(per_side)],
        put,
    )


def near(queries, keys, values):
    return held_call(
        near_kernel,
        [((LANES, ROWS), BF16), ((1, 8, ROWS), F32)],
        queries,
        keys,
        values,
        cost_estimate=pl.CostEstimate(
            flops=2 * 4 * ROWS * ROWS * HEAD_WIDTH,
            bytes_accessed=4 * ROWS * LANES * 2,
            transcendentals=2 * ROWS * ROWS,
        ),
        room=16,
        name="near",
    )


def mid_kernel(r_ref, s_ref):
    key_value = r_ref[:, 0:MID, :].reshape(ROWS, LANES)
    columns = jnp.concatenate(
        [key_value.T[HEAD_WIDTH:], jnp.ones((16, ROWS), BF16)], axis=0
    )
    low = lane_low((MID // 2, LANES))

    def query_block(source):
        packed = r_ref[source, MID : MID + MID // 2, :].astype(F32) * SCALE
        first = jnp.where(low, packed, 0.0)
        second = jnp.where(low, pltpu.roll(packed, HEAD_WIDTH, 1), 0.0)
        return jnp.concatenate([first, second], axis=0).astype(BF16)

    def query_part(step):
        return lambda: jnp.concatenate([query_block(2 * step), query_block(2 * step + 1)], axis=0)

    def put(step, mixed, lse):
        parts = [part.astype(F32) for part in split3(lse)]
        block = jnp.concatenate(
            [mixed] + parts + [jnp.zeros((BACK_MID - HEAD_WIDTH - 3, CHUNK), F32)], axis=0
        ).astype(BF16)
        s_ref[2 * step] = block[:, :MID]
        s_ref[2 * step + 1] = block[:, MID:]

    steps = ROWS // CHUNK
    chunks_of(key_value, [query_part(s) for s in range(steps)], [columns] * steps, put)


def mid(received):
    return held_call(
        mid_kernel,
        [((SEG, BACK_MID, MID), BF16)],
        received,
        cost_estimate=pl.CostEstimate(
            flops=4 * ROWS * ROWS * HEAD_WIDTH,
            bytes_accessed=ROWS * LANES * 4,
            transcendentals=ROWS * ROWS,
        ),
        room=16,
        name="mid",
    )[0]


def far_kernel(r_ref, others_ref, m_ref, s_ref, stage_ref, sems):
    early = pltpu.make_async_copy(m_ref, s_ref.at[:, 0:BACK_MID, :], sems.at[0])
    early.start()
    queries = r_ref[:, MID + MID // 2 : SEND_MID, :].astype(F32) * SCALE
    others = others_ref[...].astype(F32)
    count = SEG * FAR
    low = lane_low((count, LANES))
    lane = lax.broadcasted_iota(jnp.int32, (count, LANES), 1)
    marks = jnp.zeros((count, LANES), F32)
    pieces = []
    for pair in range(PAIRS):
        rows = queries[:, pair * FAR : (pair + 1) * FAR, :].reshape(count, LANES)
        key_rows = (
            others[:, pair * FAR : (pair + 1) * FAR, :].reshape(SLIDE_GRP * FAR, LANES).astype(BF16)
        )
        value_rows = (
            others[:, (PAIRS + pair) * FAR : (PAIRS + pair + 1) * FAR, :]
            .reshape(SLIDE_GRP * FAR, LANES)
            .astype(BF16)
        )
        outs = []
        for side in range(2):
            keep = low if side == 0 else jnp.logical_not(low)
            scores = dot(jnp.where(keep, rows, 0.0).astype(BF16), key_rows, NT)
            highest = jnp.max(scores, axis=1, keepdims=True)
            raised = jnp.exp(scores - highest)
            totals = jnp.sum(raised, axis=1, keepdims=True)
            outs.append(dot(raised.astype(BF16), value_rows, NN) / totals)
            for place, part in enumerate(split3(highest + jnp.log(totals))):
                marks = jnp.where(
                    lane == 3 * (2 * pair + side) + place, part.astype(F32), marks
                )
        pieces.append(jnp.where(low, outs[0], outs[1]).reshape(SEG, FAR, LANES))
    pieces.append(marks.reshape(SEG, FAR, LANES))
    stage_ref[...] = jnp.concatenate(pieces, axis=1).astype(BF16)
    late = pltpu.make_async_copy(stage_ref, s_ref.at[:, BACK_MID:BACK, :], sems.at[1])
    late.start()
    early.wait()
    late.wait()


def far(received, others, mid_part):
    operands = (received, others, mid_part)
    return pl.pallas_call(
        far_kernel,
        out_shape=jax.ShapeDtypeStruct((SEG, BACK, LANES), BF16),
        in_specs=[pl.BlockSpec(memory_space=pltpu.VMEM)] * len(operands),
        out_specs=pl.BlockSpec(memory_space=pl.ANY),
        scratch_shapes=[
            pltpu.VMEM((SEG, BACK - BACK_MID, LANES), BF16),
            pltpu.SemaphoreType.DMA((2,)),
        ],
        compiler_params=pltpu.CompilerParams(vmem_limit_bytes=8 * 2**20),
        name="far",
    )(*[pltpu.with_memory_space_constraint(x, pltpu.VMEM) for x in operands])


def merge_kernel(*refs):
    near_refs, lse_refs = refs[:PAIRS], refs[PAIRS : 2 * PAIRS]
    back_ref, out_ref, stage_ref, sems = refs[2 * PAIRS :]
    moves = []
    width = HEADS * HEAD_WIDTH
    parts = back_ref[:, BACK_MID:, :].astype(F32)
    count = SEG * FAR
    marks = parts[:, PAIRS * FAR :, :].reshape(count, LANES).astype(BF16)
    source = lax.broadcasted_iota(jnp.int32, (LANES, width), 0)
    target = lax.broadcasted_iota(jnp.int32, (LANES, width), 1) // HEAD_WIDTH
    gather = jnp.logical_and(source >= 3 * target, source < 3 * target + 3).astype(BF16)
    lse_parts = dot(marks, gather, NN).reshape(SEG, FAR, width)
    far_parts = jnp.concatenate(
        [
            parts[:, pair * FAR : (pair + 1) * FAR, :].reshape(count, LANES)
            for pair in range(PAIRS)
        ],
        axis=1,
    ).reshape(SEG, FAR, width)
    top = jnp.max(lse_parts, axis=0)
    weights = jnp.exp(lse_parts - top[None])
    total = jnp.sum(weights, axis=0)
    far_out = jnp.sum(weights * far_parts, axis=0) / total
    far_lse = top + jnp.log(total)
    place = lax.broadcasted_iota(jnp.int32, (FAR, MID), 0) * (MID // FAR)
    lane = lax.broadcasted_iota(jnp.int32, (FAR, MID), 1)
    thin = (lane == place).astype(BF16)
    far_rows = jnp.concatenate([far_out] + [x.astype(F32) for x in split3(far_lse)], axis=1)
    far_wide = dot(far_rows.astype(BF16), thin, TN)
    has_far = lax.broadcasted_iota(jnp.int32, (1, MID), 1) % (MID // FAR) == 0
    slot = lax.broadcasted_iota(jnp.int32, (MID, ROWS), 0) * SEG
    token = lax.broadcasted_iota(jnp.int32, (MID, ROWS), 1)
    offset = token - slot
    phase = lax.broadcasted_iota(jnp.int32, (1, ROWS), 1) % SEG
    start = 0
    for ref, lse_ref in zip(near_refs, lse_refs):
        for pair in range(ref.shape[0] // LANES):
            sides = []
            for side in range(2):
                head = start + 2 * pair + side
                back = back_ref[head, :BACK_MID].astype(F32)
                mid_out = back[:HEAD_WIDTH]
                mid_lse = back[64:65] + back[65:66] + back[66:67]
                base = head * HEAD_WIDTH
                w_out = far_wide[base : base + HEAD_WIDTH]
                w_lse = (
                    far_wide[width + base : width + base + 1]
                    + far_wide[2 * width + base : 2 * width + base + 1]
                    + far_wide[3 * width + base : 3 * width + base + 1]
                )
                w_lse = jnp.where(has_far, w_lse, mid_lse)
                high = jnp.maximum(mid_lse, w_lse)
                w_mid = jnp.exp(mid_lse - high)
                w_far = jnp.where(has_far, jnp.exp(w_lse - high), 0.0)
                sums = w_mid + w_far
                joint = (w_mid * mid_out + w_far * w_out) / sums
                joint_lse = high + jnp.log(sums)
                block = jnp.concatenate(
                    [joint]
                    + [x.astype(F32) for x in split3(joint_lse)]
                    + [jnp.zeros((BACK_MID - HEAD_WIDTH - 3, MID), F32)],
                    axis=0,
                ).astype(BF16)
                spread = dot(block, (offset == head).astype(BF16), NN)
                near_lse = lse_ref[pair, side : side + 1, :]
                joint_wide = spread[64:65] + spread[65:66] + spread[66:67]
                covered = phase == head
                joint_wide = jnp.where(covered, joint_wide, near_lse)
                ceiling = jnp.maximum(near_lse, joint_wide)
                near_weight = jnp.exp(near_lse - ceiling)
                joint_weight = jnp.where(covered, jnp.exp(joint_wide - ceiling), 0.0)
                share = joint_weight / (near_weight + joint_weight)
                rest = near_weight / (near_weight + joint_weight)
                own = ref[
                    pair * LANES + side * HEAD_WIDTH : pair * LANES + (side + 1) * HEAD_WIDTH, :
                ].astype(F32)
                sides.append(rest * own + share * spread[:HEAD_WIDTH])
            whole = start // 2 + pair
            stage_ref[whole] = jnp.concatenate(sides, axis=0).astype(BF16).T
            move = pltpu.make_async_copy(
                stage_ref.at[whole],
                out_ref.at[:, whole * LANES : (whole + 1) * LANES],
                sems.at[whole],
            )
            move.start()
            moves.append(move)
        start += 2 * (ref.shape[0] // LANES)
    for move in moves:
        move.wait()


def merge(near_outs, near_lses, back):
    operands = (*near_outs, *near_lses, back)
    return pl.pallas_call(
        merge_kernel,
        out_shape=jax.ShapeDtypeStruct((ROWS, HEADS * HEAD_WIDTH), BF16),
        in_specs=[pl.BlockSpec(memory_space=pltpu.VMEM)] * len(operands),
        out_specs=pl.BlockSpec(memory_space=pl.ANY),
        scratch_shapes=[
            pltpu.VMEM((PAIRS, ROWS, LANES), BF16),
            pltpu.SemaphoreType.DMA((PAIRS,)),
        ],
        compiler_params=pltpu.CompilerParams(vmem_limit_bytes=16 * 2**20),
        name="merge",
    )(*[pltpu.with_memory_space_constraint(x, pltpu.VMEM) for x in operands])


def body(queries, keys, values):
    size = lax.axis_size("grp")
    near_groups = [[first + i for i in range(4)] for first in range(0, size, 4)]
    held = pack_far(keys, values)
    mid_send, *pieces = pack(queries, keys, values)
    mid_got = lax.all_to_all(mid_send, "seg", 0, 0, tiled=True)
    for mask in (8, 4):
        other = lax.ppermute(held, "grp", [(i, i ^ mask) for i in range(size)])
        held = jnp.concatenate([held, other], axis=0)
    others = lax.all_to_all(
        jnp.tile(held, (4, 1, 1)), "grp", 0, 0, tiled=True, axis_index_groups=near_groups
    )
    nears = []
    for pair in range(3):
        nears.append(near(*pieces[3 * pair : 3 * pair + 3]))
    mid_part = mid(mid_got)
    part = far(mid_got, others, mid_part)
    back = lax.all_to_all(part, "seg", 0, 0, tiled=True)
    return merge([n[0] for n in nears], [n[1] for n in nears], back)


def solution(mesh):
    return jax.shard_map(
        body,
        mesh=mesh,
        in_specs=(P(("grp", "seg"), None),) * 3,
        out_specs=P(("grp", "seg"), None),
        check_vma=False,
    )
```

```python
import jax
import jax.numpy as jnp
from jax import lax
from jax.experimental import pallas as pl
from jax.experimental.pallas import tpu as pltpu
from jax.sharding import PartitionSpec as P

HEADS = 6
HEAD_WIDTH = 64
PAIRS = HEADS // 2
LANES = 2 * HEAD_WIDTH
SLIDE_GRP = 16
SEG = 8
ROWS = 1024
MID = ROWS // SEG
FAR_PERIOD = SLIDE_GRP * SEG
FAR = ROWS // FAR_PERIOD
CHUNK = 256
BLOCK = 256
SCALE = HEAD_WIDTH ** (-0.5)


NT = (((1,), (1,)), ((), ()))
NN = (((1,), (0,)), ((), ()))
TN = (((0,), (0,)), ((), ()))
F32 = jnp.float32
BF16 = jnp.bfloat16

SEND_MID = 216
BACK_MID = 72
BACK = BACK_MID + (PAIRS + 1) * FAR


def held_call(kernel, out_shapes, *operands, room=8, **options):
    outs = tuple(pltpu.VMEM(shape, dtype) for shape, dtype in out_shapes)
    space = pl.BlockSpec(memory_space=pltpu.VMEM)
    return pl.pallas_call(
        kernel,
        out_shape=outs,
        in_specs=[space] * len(operands),
        out_specs=(space,) * len(outs),
        compiler_params=pltpu.CompilerParams(vmem_limit_bytes=room * 2**20),
        **options,
    )(*[pltpu.with_memory_space_constraint(x, pltpu.VMEM) for x in operands])


def dot(a, b, dims):
    return lax.dot_general(a, b, dims, preferred_element_type=F32)


def lane_low(shape):
    return lax.broadcasted_iota(jnp.int32, shape, len(shape) - 1) < HEAD_WIDTH


def split3(x):
    high = x.astype(BF16)
    rest = x - high.astype(F32)
    middle = rest.astype(BF16)
    low = (rest - middle.astype(F32)).astype(BF16)
    return high, middle, low


def pack_far_kernel(k_ref, v_ref, far_ref, taken, wide, sems):
    moves = []
    for place, source in enumerate((k_ref, v_ref)):
        move = pltpu.make_async_copy(source.at[:, 0:SEG, :], taken.at[place], sems.at[place])
        move.start()
        moves.append(move)
    low = lane_low((FAR, LANES))
    rows = []
    for place, move in enumerate(moves):
        move.wait()
        for pair in range(PAIRS):
            lanes = slice(pair * LANES, (pair + 1) * LANES)
            wide[...] = taken[place, :, :, lanes].astype(F32).reshape(FAR * SEG, LANES)
            first = wide[pl.ds(2 * pair, FAR, stride=SEG), :]
            second = wide[pl.ds(2 * pair + 1, FAR, stride=SEG), :]
            rows.append(jnp.where(low, first, second))
    far_ref[0] = jnp.concatenate(rows, axis=0).astype(BF16)


def pack_far(keys, values):
    width = HEADS * HEAD_WIDTH
    operands = [x.reshape(FAR, FAR_PERIOD, width) for x in (keys, values)]
    return pl.pallas_call(
        pack_far_kernel,
        out_shape=pltpu.VMEM((1, 2 * PAIRS * FAR, LANES), BF16),
        in_specs=[pl.BlockSpec(memory_space=pl.ANY)] * 2,
        out_specs=pl.BlockSpec(memory_space=pltpu.VMEM),
        scratch_shapes=[
            pltpu.VMEM((2, FAR, SEG, width), BF16),
            pltpu.VMEM((FAR * SEG, LANES), F32),
            pltpu.SemaphoreType.DMA((2,)),
        ],
        compiler_params=pltpu.CompilerParams(vmem_limit_bytes=4 * 2**20),
        name="pack_far",
    )(*[pltpu.with_memory_space_constraint(x, pltpu.HBM) for x in operands])


def pack_kernel(*refs):
    sources, refs = refs[:3], refs[3:]
    mid_ref, copies, (q_wide, k_wide, v_wide, sems) = refs[0], refs[1:-4], refs[-4:]
    moves = []
    for pair in range(PAIRS):
        for place, source in enumerate(sources):
            slot = 3 * pair + place
            move = pltpu.make_async_copy(
                source.at[:, pair * LANES : (pair + 1) * LANES], copies[slot], sems.at[slot]
            )
            move.start()
            moves.append(move)
    far_q = []
    low_mid = lane_low((MID, LANES))
    low_half = lane_low((MID // 2, LANES))
    low_far = lane_low((FAR, LANES))
    for spare in range(HEADS, SEG):
        mid_ref[spare, 0 : MID + MID // 2, :] = jnp.zeros((MID + MID // 2, LANES), BF16)
    for pair in range(PAIRS):
        for place, wide in enumerate((q_wide, k_wide, v_wide)):
            moves[3 * pair + place].wait()
            wide[...] = copies[3 * pair + place][...].astype(F32)
        for side in range(2):
            head = 2 * pair + side
            q_rows = q_wide[pl.ds(head, MID, stride=SEG), :]
            k_rows = k_wide[pl.ds(head, MID, stride=SEG), :]
            v_rows = v_wide[pl.ds(head, MID, stride=SEG), :]
            if side == 0:
                key_value = jnp.where(low_mid, k_rows, pltpu.roll(v_rows, HEAD_WIDTH, 1))
                query = jnp.where(
                    low_half, q_rows[: MID // 2], pltpu.roll(q_rows[MID // 2 :], HEAD_WIDTH, 1)
                )
            else:
                key_value = jnp.where(low_mid, pltpu.roll(k_rows, HEAD_WIDTH, 1), v_rows)
                query = jnp.where(
                    low_half, pltpu.roll(q_rows[: MID // 2], HEAD_WIDTH, 1), q_rows[MID // 2 :]
                )
            mid_ref[head, 0:MID, :] = key_value.astype(BF16)
            mid_ref[head, MID : MID + MID // 2, :] = query.astype(BF16)
        first = q_wide[pl.ds(2 * pair, FAR, stride=FAR_PERIOD), :]
        second = q_wide[pl.ds(2 * pair + 1, FAR, stride=FAR_PERIOD), :]
        far_q.append(jnp.where(low_far, first, second))
    tail = jnp.concatenate(far_q, axis=0).astype(BF16)
    for target in range(SEG):
        mid_ref[target, MID + MID // 2 : SEND_MID, :] = tail


def pack(queries, keys, values):
    shapes = [((SEG, SEND_MID, LANES), BF16)] + [((ROWS, LANES), BF16)] * (3 * PAIRS)
    space = pl.BlockSpec(memory_space=pltpu.VMEM)
    return pl.pallas_call(
        pack_kernel,
        out_shape=tuple(pltpu.VMEM(shape, dtype) for shape, dtype in shapes),
        in_specs=[pl.BlockSpec(memory_space=pl.ANY)] * 3,
        out_specs=(space,) * len(shapes),
        scratch_shapes=[pltpu.VMEM((ROWS, LANES), F32)] * 3
        + [pltpu.SemaphoreType.DMA((3 * PAIRS,))],
        compiler_params=pltpu.CompilerParams(vmem_limit_bytes=8 * 2**20),
        name="pack",
    )(*[pltpu.with_memory_space_constraint(x, pltpu.HBM) for x in (queries, keys, values)])


def chunks_of(key_rows, query_parts, value_parts, put):
    count = len(query_parts)
    blocks = [slice(at, at + BLOCK) for at in range(0, ROWS, BLOCK)]

    def top_of(tiles):
        best = tiles[0]
        for tile in tiles[1:]:
            best = jnp.maximum(best, tile)
        return jnp.max(best, axis=0, keepdims=True)

    query = query_parts[0]()
    pending = [dot(key_rows[block], query, NT) for block in blocks]
    for step in range(count):
        highest = top_of(pending)
        query = query_parts[step + 1]() if step + 1 < count else None
        following, mixed = [], None
        raised = []
        for block, tile in zip(blocks, pending):
            if query is not None:
                following.append(dot(key_rows[block], query, NT))
            raised.append(jnp.exp(tile - highest).astype(BF16))
        mixed = dot(value_parts[step], jnp.concatenate(raised, axis=0), NN)
        totals = mixed[HEAD_WIDTH : HEAD_WIDTH + 1]
        put(step, mixed[:HEAD_WIDTH] / totals, highest + jnp.log(totals))
        pending = following


def near_kernel(q_ref, k_ref, v_ref, o_ref, l_ref):
    key_rows = k_ref[...]
    columns = v_ref[...].T
    ones = jnp.ones((16, ROWS), BF16)
    sides = [
        jnp.concatenate([columns[i * HEAD_WIDTH : (i + 1) * HEAD_WIDTH], ones], axis=0)
        for i in range(2)
    ]
    low = lane_low((CHUNK, LANES))
    per_side = ROWS // CHUNK

    def query_part(side, part):
        def get():
            rows = q_ref[part * CHUNK : (part + 1) * CHUNK, :] * BF16(SCALE)
            keep = low if side == 0 else jnp.logical_not(low)
            return jnp.where(keep, rows, BF16(0))

        return get

    def put(step, mixed, lse):
        side, part = step // per_side, step % per_side
        span = slice(part * CHUNK, (part + 1) * CHUNK)
        o_ref[side * HEAD_WIDTH : (side + 1) * HEAD_WIDTH, span] = mixed.astype(BF16)
        l_ref[0, side : side + 1, span] = lse

    chunks_of(
        key_rows,
        [query_part(s, p) for s in range(2) for p in range(per_side)],
        [sides[s] for s in range(2) for _ in range(per_side)],
        put,
    )


def near(queries, keys, values):
    return held_call(
        near_kernel,
        [((LANES, ROWS), BF16), ((1, 8, ROWS), F32)],
        queries,
        keys,
        values,
        cost_estimate=pl.CostEstimate(
            flops=2 * 4 * ROWS * ROWS * HEAD_WIDTH,
            bytes_accessed=4 * ROWS * LANES * 2,
            transcendentals=2 * ROWS * ROWS,
        ),
        room=16,
        name="near",
    )


def mid_kernel(r_ref, s_ref):
    key_value = r_ref[:, 0:MID, :].reshape(ROWS, LANES)
    columns = jnp.concatenate(
        [key_value.T[HEAD_WIDTH:], jnp.ones((16, ROWS), BF16)], axis=0
    )
    low = lane_low((MID // 2, LANES))

    def query_block(source):
        packed = r_ref[source, MID : MID + MID // 2, :].astype(F32) * SCALE
        first = jnp.where(low, packed, 0.0)
        second = jnp.where(low, pltpu.roll(packed, HEAD_WIDTH, 1), 0.0)
        return jnp.concatenate([first, second], axis=0).astype(BF16)

    def query_part(step):
        return lambda: jnp.concatenate([query_block(2 * step), query_block(2 * step + 1)], axis=0)

    def put(step, mixed, lse):
        parts = [part.astype(F32) for part in split3(lse)]
        block = jnp.concatenate(
            [mixed] + parts + [jnp.zeros((BACK_MID - HEAD_WIDTH - 3, CHUNK), F32)], axis=0
        ).astype(BF16)
        s_ref[2 * step] = block[:, :MID]
        s_ref[2 * step + 1] = block[:, MID:]

    steps = ROWS // CHUNK
    chunks_of(key_value, [query_part(s) for s in range(steps)], [columns] * steps, put)


def mid(received):
    return held_call(
        mid_kernel,
        [((SEG, BACK_MID, MID), BF16)],
        received,
        cost_estimate=pl.CostEstimate(
            flops=4 * ROWS * ROWS * HEAD_WIDTH,
            bytes_accessed=ROWS * LANES * 4,
            transcendentals=ROWS * ROWS,
        ),
        room=16,
        name="mid",
    )[0]


def far_kernel(r_ref, others_ref, m_ref, s_ref, stage_ref, sems):
    early = pltpu.make_async_copy(m_ref, s_ref.at[:, 0:BACK_MID, :], sems.at[0])
    early.start()
    queries = r_ref[:, MID + MID // 2 : SEND_MID, :].astype(F32) * SCALE
    others = others_ref[...].astype(F32)
    count = SEG * FAR
    low = lane_low((count, LANES))
    lane = lax.broadcasted_iota(jnp.int32, (count, LANES), 1)
    tiles, value_sides = [], []
    for pair in range(PAIRS):
        rows = queries[:, pair * FAR : (pair + 1) * FAR, :].reshape(count, LANES)
        key_rows = (
            others[:, pair * FAR : (pair + 1) * FAR, :].reshape(SLIDE_GRP * FAR, LANES).astype(BF16)
        )
        value_sides.append(
            others[:, (PAIRS + pair) * FAR : (PAIRS + pair + 1) * FAR, :]
            .reshape(SLIDE_GRP * FAR, LANES)
            .astype(BF16)
        )
        both = jnp.concatenate([jnp.where(low, rows, 0.0), jnp.where(low, 0.0, rows)], axis=0)
        tiles.append(dot(both.astype(BF16), key_rows, NT))
    scores = jnp.concatenate(tiles, axis=0)
    highest = jnp.max(scores, axis=1, keepdims=True)
    raised = jnp.exp(scores - highest).astype(BF16)
    totals = dot(raised, jnp.ones((SLIDE_GRP * FAR, LANES), BF16), NN)
    parts = [part.astype(F32) for part in split3(highest + jnp.log(totals))]
    marks = jnp.zeros((count, LANES), F32)
    pieces = []
    for pair in range(PAIRS):
        span = slice(2 * pair * count, 2 * (pair + 1) * count)
        mixed = dot(raised[span], value_sides[pair], NN) / totals[span]
        pieces.append(jnp.where(low, mixed[:count], mixed[count:]).reshape(SEG, FAR, LANES))
        for side in range(2):
            head = 2 * pair + side
            for place, part in enumerate(parts):
                marks = jnp.where(
                    lane == 3 * head + place, part[head * count : (head + 1) * count], marks
                )
    pieces.append(marks.reshape(SEG, FAR, LANES))
    stage_ref[...] = jnp.concatenate(pieces, axis=1).astype(BF16)
    late = pltpu.make_async_copy(stage_ref, s_ref.at[:, BACK_MID:BACK, :], sems.at[1])
    late.start()
    early.wait()
    late.wait()


def far(received, others, mid_part):
    operands = (received, others, mid_part)
    return pl.pallas_call(
        far_kernel,
        out_shape=jax.ShapeDtypeStruct((SEG, BACK, LANES), BF16),
        in_specs=[pl.BlockSpec(memory_space=pltpu.VMEM)] * len(operands),
        out_specs=pl.BlockSpec(memory_space=pl.ANY),
        scratch_shapes=[
            pltpu.VMEM((SEG, BACK - BACK_MID, LANES), BF16),
            pltpu.SemaphoreType.DMA((2,)),
        ],
        compiler_params=pltpu.CompilerParams(vmem_limit_bytes=8 * 2**20),
        name="far",
    )(*[pltpu.with_memory_space_constraint(x, pltpu.VMEM) for x in operands])


def maps_kernel(o_ref):
    slot = lax.broadcasted_iota(jnp.int32, (MID, ROWS), 0) * SEG
    offset = lax.broadcasted_iota(jnp.int32, (MID, ROWS), 1) - slot
    for head in range(HEADS):
        o_ref[head] = (offset == head).astype(BF16)


def maps():
    return held_call(maps_kernel, [((HEADS, MID, ROWS), BF16)], name="maps")[0]


def merge_kernel(*refs):
    near_refs, lse_refs = refs[:PAIRS], refs[PAIRS : 2 * PAIRS]
    back_ref, map_ref, out_ref, stage_ref, sems = refs[2 * PAIRS :]
    moves = []
    width = HEADS * HEAD_WIDTH
    parts = back_ref[:, BACK_MID:, :].astype(F32)
    count = SEG * FAR
    marks = parts[:, PAIRS * FAR :, :].reshape(count, LANES).astype(BF16)
    source = lax.broadcasted_iota(jnp.int32, (LANES, width), 0)
    target = lax.broadcasted_iota(jnp.int32, (LANES, width), 1) // HEAD_WIDTH
    gather = jnp.logical_and(source >= 3 * target, source < 3 * target + 3).astype(BF16)
    lse_parts = dot(marks, gather, NN).reshape(SEG, FAR, width)
    far_parts = jnp.concatenate(
        [
            parts[:, pair * FAR : (pair + 1) * FAR, :].reshape(count, LANES)
            for pair in range(PAIRS)
        ],
        axis=1,
    ).reshape(SEG, FAR, width)
    top = jnp.max(lse_parts, axis=0)
    weights = jnp.exp(lse_parts - top[None])
    total = jnp.sum(weights, axis=0)
    far_out = jnp.sum(weights * far_parts, axis=0) / total
    far_lse = top + jnp.log(total)
    place = lax.broadcasted_iota(jnp.int32, (FAR, MID), 0) * (MID // FAR)
    lane = lax.broadcasted_iota(jnp.int32, (FAR, MID), 1)
    thin = (lane == place).astype(BF16)
    far_rows = jnp.concatenate([far_out] + [x.astype(F32) for x in split3(far_lse)], axis=1)
    far_wide = dot(far_rows.astype(BF16), thin, TN)
    has_far = lax.broadcasted_iota(jnp.int32, (1, MID), 1) % (MID // FAR) == 0
    phase = lax.broadcasted_iota(jnp.int32, (1, ROWS), 1) % SEG
    start = 0
    for ref, lse_ref in zip(near_refs, lse_refs):
        for pair in range(ref.shape[0] // LANES):
            sides = []
            for side in range(2):
                head = start + 2 * pair + side
                back = back_ref[head, :BACK_MID].astype(F32)
                mid_out = back[:HEAD_WIDTH]
                mid_lse = back[64:65] + back[65:66] + back[66:67]
                base = head * HEAD_WIDTH
                w_out = far_wide[base : base + HEAD_WIDTH]
                w_lse = (
                    far_wide[width + base : width + base + 1]
                    + far_wide[2 * width + base : 2 * width + base + 1]
                    + far_wide[3 * width + base : 3 * width + base + 1]
                )
                w_lse = jnp.where(has_far, w_lse, mid_lse)
                high = jnp.maximum(mid_lse, w_lse)
                w_mid = jnp.exp(mid_lse - high)
                w_far = jnp.where(has_far, jnp.exp(w_lse - high), 0.0)
                sums = w_mid + w_far
                joint = (w_mid * mid_out + w_far * w_out) / sums
                joint_lse = high + jnp.log(sums)
                block = jnp.concatenate(
                    [joint]
                    + [x.astype(F32) for x in split3(joint_lse)]
                    + [jnp.zeros((BACK_MID - HEAD_WIDTH - 3, MID), F32)],
                    axis=0,
                ).astype(BF16)
                spread = dot(block, map_ref[head], NN)
                near_lse = lse_ref[pair, side : side + 1, :]
                joint_wide = spread[64:65] + spread[65:66] + spread[66:67]
                covered = phase == head
                joint_wide = jnp.where(covered, joint_wide, near_lse)
                ceiling = jnp.maximum(near_lse, joint_wide)
                near_weight = jnp.exp(near_lse - ceiling)
                joint_weight = jnp.where(covered, jnp.exp(joint_wide - ceiling), 0.0)
                share = joint_weight / (near_weight + joint_weight)
                rest = near_weight / (near_weight + joint_weight)
                own = ref[
                    pair * LANES + side * HEAD_WIDTH : pair * LANES + (side + 1) * HEAD_WIDTH, :
                ].astype(F32)
                sides.append(rest * own + share * spread[:HEAD_WIDTH])
            whole = start // 2 + pair
            stage_ref[whole] = jnp.concatenate(sides, axis=0).astype(BF16).T
            move = pltpu.make_async_copy(
                stage_ref.at[whole],
                out_ref.at[:, whole * LANES : (whole + 1) * LANES],
                sems.at[whole],
            )
            move.start()
            moves.append(move)
        start += 2 * (ref.shape[0] // LANES)
    for move in moves:
        move.wait()


def merge(near_outs, near_lses, back, places):
    operands = (*near_outs, *near_lses, back, places)
    return pl.pallas_call(
        merge_kernel,
        out_shape=jax.ShapeDtypeStruct((ROWS, HEADS * HEAD_WIDTH), BF16),
        in_specs=[pl.BlockSpec(memory_space=pltpu.VMEM)] * len(operands),
        out_specs=pl.BlockSpec(memory_space=pl.ANY),
        scratch_shapes=[
            pltpu.VMEM((PAIRS, ROWS, LANES), BF16),
            pltpu.SemaphoreType.DMA((PAIRS,)),
        ],
        compiler_params=pltpu.CompilerParams(vmem_limit_bytes=16 * 2**20),
        name="merge",
    )(*[pltpu.with_memory_space_constraint(x, pltpu.VMEM) for x in operands])


def body(queries, keys, values):
    size = lax.axis_size("grp")
    near_groups = [[first + i for i in range(4)] for first in range(0, size, 4)]
    held = pack_far(keys, values)
    mid_send, *pieces = pack(queries, keys, values)
    mid_got = lax.all_to_all(mid_send, "seg", 0, 0, tiled=True)
    for mask in (8, 4):
        other = lax.ppermute(held, "grp", [(i, i ^ mask) for i in range(size)])
        held = jnp.concatenate([held, other], axis=0)
    others = lax.all_to_all(
        jnp.tile(held, (4, 1, 1)), "grp", 0, 0, tiled=True, axis_index_groups=near_groups
    )
    nears = []
    for pair in range(3):
        nears.append(near(*pieces[3 * pair : 3 * pair + 3]))
    mid_part = mid(mid_got)
    part = far(mid_got, others, mid_part)
    back = lax.all_to_all(part, "seg", 0, 0, tiled=True)
    places = maps()
    return merge([n[0] for n in nears], [n[1] for n in nears], back, places)


def solution(mesh):
    return jax.shard_map(
        body,
        mesh=mesh,
        in_specs=(P(("grp", "seg"), None),) * 3,
        out_specs=P(("grp", "seg"), None),
        check_vma=False,
    )
```

```python
import jax
import jax.numpy as jnp
from jax import lax
from jax.experimental import pallas as pl
from jax.experimental.pallas import tpu as pltpu
from jax.sharding import PartitionSpec as P

HEADS = 6
HEAD_WIDTH = 64
PAIRS = HEADS // 2
LANES = 2 * HEAD_WIDTH
SLIDE_GRP = 16
SEG = 8
ROWS = 1024
MID = ROWS // SEG
FAR_PERIOD = SLIDE_GRP * SEG
FAR = ROWS // FAR_PERIOD
CHUNK = 256
BLOCK = 256
SCALE = HEAD_WIDTH ** (-0.5)


NT = (((1,), (1,)), ((), ()))
NN = (((1,), (0,)), ((), ()))
TN = (((0,), (0,)), ((), ()))
F32 = jnp.float32
BF16 = jnp.bfloat16

SEND_MID = 216
BACK_MID = 72
BACK = BACK_MID + (PAIRS + 1) * FAR


def held_call(kernel, out_shapes, *operands, room=8, **options):
    outs = tuple(pltpu.VMEM(shape, dtype) for shape, dtype in out_shapes)
    space = pl.BlockSpec(memory_space=pltpu.VMEM)
    return pl.pallas_call(
        kernel,
        out_shape=outs,
        in_specs=[space] * len(operands),
        out_specs=(space,) * len(outs),
        compiler_params=pltpu.CompilerParams(vmem_limit_bytes=room * 2**20),
        **options,
    )(*[pltpu.with_memory_space_constraint(x, pltpu.VMEM) for x in operands])


def dot(a, b, dims):
    return lax.dot_general(a, b, dims, preferred_element_type=F32)


def lane_low(shape):
    return lax.broadcasted_iota(jnp.int32, shape, len(shape) - 1) < HEAD_WIDTH


def split3(x):
    high = x.astype(BF16)
    rest = x - high.astype(F32)
    middle = rest.astype(BF16)
    low = (rest - middle.astype(F32)).astype(BF16)
    return high, middle, low


def pack_kernel(*refs):
    sources, refs = refs[:3], refs[3:]
    mid_ref, far_ref = refs[:2]
    copies, (q_wide, k_wide, v_wide, sems) = refs[2:-4], refs[-4:]
    moves = []
    for pair in range(PAIRS):
        for place, source in enumerate(sources):
            slot = 3 * pair + place
            move = pltpu.make_async_copy(
                source.at[:, pair * LANES : (pair + 1) * LANES], copies[slot], sems.at[slot]
            )
            move.start()
            moves.append(move)
    far_q, far_k, far_v = [], [], []
    low_mid = lane_low((MID, LANES))
    low_half = lane_low((MID // 2, LANES))
    low_far = lane_low((FAR, LANES))
    for spare in range(HEADS, SEG):
        mid_ref[spare, 0 : MID + MID // 2, :] = jnp.zeros((MID + MID // 2, LANES), BF16)
    for pair in range(PAIRS):
        for place, wide in enumerate((q_wide, k_wide, v_wide)):
            moves[3 * pair + place].wait()
            wide[...] = copies[3 * pair + place][...].astype(F32)
        for side in range(2):
            head = 2 * pair + side
            q_rows = q_wide[pl.ds(head, MID, stride=SEG), :]
            k_rows = k_wide[pl.ds(head, MID, stride=SEG), :]
            v_rows = v_wide[pl.ds(head, MID, stride=SEG), :]
            if side == 0:
                key_value = jnp.where(low_mid, k_rows, pltpu.roll(v_rows, HEAD_WIDTH, 1))
                query = jnp.where(
                    low_half, q_rows[: MID // 2], pltpu.roll(q_rows[MID // 2 :], HEAD_WIDTH, 1)
                )
            else:
                key_value = jnp.where(low_mid, pltpu.roll(k_rows, HEAD_WIDTH, 1), v_rows)
                query = jnp.where(
                    low_half, pltpu.roll(q_rows[: MID // 2], HEAD_WIDTH, 1), q_rows[MID // 2 :]
                )
            mid_ref[head, 0:MID, :] = key_value.astype(BF16)
            mid_ref[head, MID : MID + MID // 2, :] = query.astype(BF16)
        for wide, out in ((q_wide, far_q), (k_wide, far_k), (v_wide, far_v)):
            first = wide[pl.ds(2 * pair, FAR, stride=FAR_PERIOD), :]
            second = wide[pl.ds(2 * pair + 1, FAR, stride=FAR_PERIOD), :]
            out.append(jnp.where(low_far, first, second))
    tail = jnp.concatenate(far_q, axis=0).astype(BF16)
    for target in range(SEG):
        mid_ref[target, MID + MID // 2 : SEND_MID, :] = tail
    far_ref[0] = jnp.concatenate(far_k + far_v, axis=0).astype(BF16)


def pack(queries, keys, values):
    shapes = [((SEG, SEND_MID, LANES), BF16), ((1, 2 * PAIRS * FAR, LANES), BF16)]
    shapes += [((ROWS, LANES), BF16)] * (3 * PAIRS)
    space = pl.BlockSpec(memory_space=pltpu.VMEM)
    return pl.pallas_call(
        pack_kernel,
        out_shape=tuple(pltpu.VMEM(shape, dtype) for shape, dtype in shapes),
        in_specs=[pl.BlockSpec(memory_space=pl.ANY)] * 3,
        out_specs=(space,) * len(shapes),
        scratch_shapes=[pltpu.VMEM((ROWS, LANES), F32)] * 3
        + [pltpu.SemaphoreType.DMA((3 * PAIRS,))],
        compiler_params=pltpu.CompilerParams(vmem_limit_bytes=8 * 2**20),
        name="pack",
    )(*[pltpu.with_memory_space_constraint(x, pltpu.HBM) for x in (queries, keys, values)])


def chunks_of(key_rows, query_parts, value_parts, put):
    count = len(query_parts)
    blocks = [slice(at, at + BLOCK) for at in range(0, ROWS, BLOCK)]

    def top_of(tiles):
        best = tiles[0]
        for tile in tiles[1:]:
            best = jnp.maximum(best, tile)
        return jnp.max(best, axis=0, keepdims=True)

    query = query_parts[0]()
    pending = [dot(key_rows[block], query, NT) for block in blocks]
    for step in range(count):
        highest = top_of(pending)
        query = query_parts[step + 1]() if step + 1 < count else None
        following, mixed = [], None
        raised = []
        for block, tile in zip(blocks, pending):
            if query is not None:
                following.append(dot(key_rows[block], query, NT))
            raised.append(jnp.exp(tile - highest).astype(BF16))
        mixed = dot(value_parts[step], jnp.concatenate(raised, axis=0), NN)
        totals = mixed[HEAD_WIDTH : HEAD_WIDTH + 1]
        put(step, mixed[:HEAD_WIDTH] / totals, highest + jnp.log(totals))
        pending = following


def near_kernel(q_ref, k_ref, v_ref, o_ref, l_ref):
    key_rows = k_ref[...]
    columns = v_ref[...].T
    ones = jnp.ones((16, ROWS), BF16)
    sides = [
        jnp.concatenate([columns[i * HEAD_WIDTH : (i + 1) * HEAD_WIDTH], ones], axis=0)
        for i in range(2)
    ]
    low = lane_low((CHUNK, LANES))
    per_side = ROWS // CHUNK

    def query_part(side, part):
        def get():
            rows = q_ref[part * CHUNK : (part + 1) * CHUNK, :] * BF16(SCALE)
            keep = low if side == 0 else jnp.logical_not(low)
            return jnp.where(keep, rows, BF16(0))

        return get

    def put(step, mixed, lse):
        side, part = step // per_side, step % per_side
        span = slice(part * CHUNK, (part + 1) * CHUNK)
        o_ref[side * HEAD_WIDTH : (side + 1) * HEAD_WIDTH, span] = mixed.astype(BF16)
        l_ref[0, side : side + 1, span] = lse

    chunks_of(
        key_rows,
        [query_part(s, p) for s in range(2) for p in range(per_side)],
        [sides[s] for s in range(2) for _ in range(per_side)],
        put,
    )


def near(queries, keys, values):
    return held_call(
        near_kernel,
        [((LANES, ROWS), BF16), ((1, 8, ROWS), F32)],
        queries,
        keys,
        values,
        cost_estimate=pl.CostEstimate(
            flops=2 * 4 * ROWS * ROWS * HEAD_WIDTH,
            bytes_accessed=4 * ROWS * LANES * 2,
            transcendentals=2 * ROWS * ROWS,
        ),
        room=16,
        name="near",
    )


def mid_kernel(r_ref, s_ref):
    key_value = r_ref[:, 0:MID, :].reshape(ROWS, LANES)
    columns = jnp.concatenate(
        [key_value.T[HEAD_WIDTH:], jnp.ones((16, ROWS), BF16)], axis=0
    )
    low = lane_low((MID // 2, LANES))

    def query_block(source):
        packed = r_ref[source, MID : MID + MID // 2, :].astype(F32) * SCALE
        first = jnp.where(low, packed, 0.0)
        second = jnp.where(low, pltpu.roll(packed, HEAD_WIDTH, 1), 0.0)
        return jnp.concatenate([first, second], axis=0).astype(BF16)

    def query_part(step):
        return lambda: jnp.concatenate([query_block(2 * step), query_block(2 * step + 1)], axis=0)

    def put(step, mixed, lse):
        parts = [part.astype(F32) for part in split3(lse)]
        block = jnp.concatenate(
            [mixed] + parts + [jnp.zeros((BACK_MID - HEAD_WIDTH - 3, CHUNK), F32)], axis=0
        ).astype(BF16)
        s_ref[2 * step] = block[:, :MID]
        s_ref[2 * step + 1] = block[:, MID:]

    steps = ROWS // CHUNK
    chunks_of(key_value, [query_part(s) for s in range(steps)], [columns] * steps, put)


def mid(received):
    return held_call(
        mid_kernel,
        [((SEG, BACK_MID, MID), BF16)],
        received,
        cost_estimate=pl.CostEstimate(
            flops=4 * ROWS * ROWS * HEAD_WIDTH,
            bytes_accessed=ROWS * LANES * 4,
            transcendentals=ROWS * ROWS,
        ),
        room=16,
        name="mid",
    )[0]


def far_kernel(r_ref, others_ref, m_ref, s_ref, stage_ref, sems):
    early = pltpu.make_async_copy(m_ref, s_ref.at[:, 0:BACK_MID, :], sems.at[0])
    early.start()
    queries = r_ref[:, MID + MID // 2 : SEND_MID, :].astype(F32) * SCALE
    others = others_ref[...].astype(F32)
    count = SEG * FAR
    low = lane_low((count, LANES))
    lane = lax.broadcasted_iota(jnp.int32, (count, LANES), 1)
    tiles, value_sides = [], []
    for pair in range(PAIRS):
        rows = queries[:, pair * FAR : (pair + 1) * FAR, :].reshape(count, LANES)
        key_rows = (
            others[:, pair * FAR : (pair + 1) * FAR, :].reshape(SLIDE_GRP * FAR, LANES).astype(BF16)
        )
        value_sides.append(
            others[:, (PAIRS + pair) * FAR : (PAIRS + pair + 1) * FAR, :]
            .reshape(SLIDE_GRP * FAR, LANES)
            .astype(BF16)
        )
        both = jnp.concatenate([jnp.where(low, rows, 0.0), jnp.where(low, 0.0, rows)], axis=0)
        tiles.append(dot(both.astype(BF16), key_rows, NT))
    scores = jnp.concatenate(tiles, axis=0)
    highest = jnp.max(scores, axis=1, keepdims=True)
    raised = jnp.exp(scores - highest).astype(BF16)
    totals = dot(raised, jnp.ones((SLIDE_GRP * FAR, LANES), BF16), NN)
    parts = [part.astype(F32) for part in split3(highest + jnp.log(totals))]
    marks = jnp.zeros((count, LANES), F32)
    pieces = []
    for pair in range(PAIRS):
        span = slice(2 * pair * count, 2 * (pair + 1) * count)
        mixed = dot(raised[span], value_sides[pair], NN) / totals[span]
        pieces.append(jnp.where(low, mixed[:count], mixed[count:]).reshape(SEG, FAR, LANES))
        for side in range(2):
            head = 2 * pair + side
            for place, part in enumerate(parts):
                marks = jnp.where(
                    lane == 3 * head + place, part[head * count : (head + 1) * count], marks
                )
    pieces.append(marks.reshape(SEG, FAR, LANES))
    stage_ref[...] = jnp.concatenate(pieces, axis=1).astype(BF16)
    late = pltpu.make_async_copy(stage_ref, s_ref.at[:, BACK_MID:BACK, :], sems.at[1])
    late.start()
    early.wait()
    late.wait()


def far(received, others, mid_part):
    operands = (received, others, mid_part)
    return pl.pallas_call(
        far_kernel,
        out_shape=jax.ShapeDtypeStruct((SEG, BACK, LANES), BF16),
        in_specs=[pl.BlockSpec(memory_space=pltpu.VMEM)] * len(operands),
        out_specs=pl.BlockSpec(memory_space=pl.ANY),
        scratch_shapes=[
            pltpu.VMEM((SEG, BACK - BACK_MID, LANES), BF16),
            pltpu.SemaphoreType.DMA((2,)),
        ],
        compiler_params=pltpu.CompilerParams(vmem_limit_bytes=8 * 2**20),
        name="far",
    )(*[pltpu.with_memory_space_constraint(x, pltpu.VMEM) for x in operands])


def maps_kernel(o_ref):
    slot = lax.broadcasted_iota(jnp.int32, (MID, ROWS), 0) * SEG
    offset = lax.broadcasted_iota(jnp.int32, (MID, ROWS), 1) - slot
    for head in range(HEADS):
        o_ref[head] = (offset == head).astype(BF16)


def maps():
    return held_call(maps_kernel, [((HEADS, MID, ROWS), BF16)], name="maps")[0]


def merge_kernel(*refs):
    near_refs, lse_refs = refs[:PAIRS], refs[PAIRS : 2 * PAIRS]
    back_ref, map_ref, out_ref, stage_ref, sems = refs[2 * PAIRS :]
    moves = []
    width = HEADS * HEAD_WIDTH
    parts = back_ref[:, BACK_MID:, :].astype(F32)
    count = SEG * FAR
    marks = parts[:, PAIRS * FAR :, :].reshape(count, LANES).astype(BF16)
    source = lax.broadcasted_iota(jnp.int32, (LANES, width), 0)
    target = lax.broadcasted_iota(jnp.int32, (LANES, width), 1) // HEAD_WIDTH
    gather = jnp.logical_and(source >= 3 * target, source < 3 * target + 3).astype(BF16)
    lse_parts = dot(marks, gather, NN).reshape(SEG, FAR, width)
    far_parts = jnp.concatenate(
        [
            parts[:, pair * FAR : (pair + 1) * FAR, :].reshape(count, LANES)
            for pair in range(PAIRS)
        ],
        axis=1,
    ).reshape(SEG, FAR, width)
    top = jnp.max(lse_parts, axis=0)
    weights = jnp.exp(lse_parts - top[None])
    total = jnp.sum(weights, axis=0)
    far_out = jnp.sum(weights * far_parts, axis=0) / total
    far_lse = top + jnp.log(total)
    place = lax.broadcasted_iota(jnp.int32, (FAR, MID), 0) * (MID // FAR)
    lane = lax.broadcasted_iota(jnp.int32, (FAR, MID), 1)
    thin = (lane == place).astype(BF16)
    far_rows = jnp.concatenate([far_out] + [x.astype(F32) for x in split3(far_lse)], axis=1)
    far_wide = dot(far_rows.astype(BF16), thin, TN)
    has_far = lax.broadcasted_iota(jnp.int32, (1, MID), 1) % (MID // FAR) == 0
    phase = lax.broadcasted_iota(jnp.int32, (1, ROWS), 1) % SEG
    start = 0
    for ref, lse_ref in zip(near_refs, lse_refs):
        for pair in range(ref.shape[0] // LANES):
            sides = []
            for side in range(2):
                head = start + 2 * pair + side
                back = back_ref[head, :BACK_MID].astype(F32)
                mid_out = back[:HEAD_WIDTH]
                mid_lse = back[64:65] + back[65:66] + back[66:67]
                base = head * HEAD_WIDTH
                w_out = far_wide[base : base + HEAD_WIDTH]
                w_lse = (
                    far_wide[width + base : width + base + 1]
                    + far_wide[2 * width + base : 2 * width + base + 1]
                    + far_wide[3 * width + base : 3 * width + base + 1]
                )
                w_lse = jnp.where(has_far, w_lse, mid_lse)
                high = jnp.maximum(mid_lse, w_lse)
                w_mid = jnp.exp(mid_lse - high)
                w_far = jnp.where(has_far, jnp.exp(w_lse - high), 0.0)
                sums = w_mid + w_far
                joint = (w_mid * mid_out + w_far * w_out) / sums
                joint_lse = high + jnp.log(sums)
                block = jnp.concatenate(
                    [joint]
                    + [x.astype(F32) for x in split3(joint_lse)]
                    + [jnp.zeros((BACK_MID - HEAD_WIDTH - 3, MID), F32)],
                    axis=0,
                ).astype(BF16)
                spread = dot(block, map_ref[head], NN)
                near_lse = lse_ref[pair, side : side + 1, :]
                joint_wide = spread[64:65] + spread[65:66] + spread[66:67]
                covered = phase == head
                joint_wide = jnp.where(covered, joint_wide, near_lse)
                ceiling = jnp.maximum(near_lse, joint_wide)
                near_weight = jnp.exp(near_lse - ceiling)
                joint_weight = jnp.where(covered, jnp.exp(joint_wide - ceiling), 0.0)
                share = joint_weight / (near_weight + joint_weight)
                rest = near_weight / (near_weight + joint_weight)
                own = ref[
                    pair * LANES + side * HEAD_WIDTH : pair * LANES + (side + 1) * HEAD_WIDTH, :
                ].astype(F32)
                sides.append(rest * own + share * spread[:HEAD_WIDTH])
            whole = start // 2 + pair
            stage_ref[whole] = jnp.concatenate(sides, axis=0).astype(BF16).T
            move = pltpu.make_async_copy(
                stage_ref.at[whole],
                out_ref.at[:, whole * LANES : (whole + 1) * LANES],
                sems.at[whole],
            )
            move.start()
            moves.append(move)
        start += 2 * (ref.shape[0] // LANES)
    for move in moves:
        move.wait()


def merge(near_outs, near_lses, back, places):
    operands = (*near_outs, *near_lses, back, places)
    return pl.pallas_call(
        merge_kernel,
        out_shape=jax.ShapeDtypeStruct((ROWS, HEADS * HEAD_WIDTH), BF16),
        in_specs=[pl.BlockSpec(memory_space=pltpu.VMEM)] * len(operands),
        out_specs=pl.BlockSpec(memory_space=pl.ANY),
        scratch_shapes=[
            pltpu.VMEM((PAIRS, ROWS, LANES), BF16),
            pltpu.SemaphoreType.DMA((PAIRS,)),
        ],
        compiler_params=pltpu.CompilerParams(vmem_limit_bytes=16 * 2**20),
        name="merge",
    )(*[pltpu.with_memory_space_constraint(x, pltpu.VMEM) for x in operands])


def body(queries, keys, values):
    size = lax.axis_size("grp")
    near_groups = [[first + i for i in range(4)] for first in range(0, size, 4)]
    mid_send, held, *pieces = pack(queries, keys, values)
    mid_got = lax.all_to_all(mid_send, "seg", 0, 0, tiled=True)
    for mask in (8, 4):
        other = lax.ppermute(held, "grp", [(i, i ^ mask) for i in range(size)])
        held = jnp.concatenate([held, other], axis=0)
    others = lax.all_to_all(
        jnp.tile(held, (4, 1, 1)), "grp", 0, 0, tiled=True, axis_index_groups=near_groups
    )
    nears = []
    for pair in range(3):
        nears.append(near(*pieces[3 * pair : 3 * pair + 3]))
    mid_part = mid(mid_got)
    part = far(mid_got, others, mid_part)
    back = lax.all_to_all(part, "seg", 0, 0, tiled=True)
    places = maps()
    return merge([n[0] for n in nears], [n[1] for n in nears], back, places)


def solution(mesh):
    return jax.shard_map(
        body,
        mesh=mesh,
        in_specs=(P(("grp", "seg"), None),) * 3,
        out_specs=P(("grp", "seg"), None),
        check_vma=False,
    )
```
